32 devices in a mesh: seg: 32 (over z, y, x, core).
Axes of the slice: x: 2, y: 2, z: 4, core: 2. Of those that a mesh axis runs over, the one named last changes fastest.
Arguments:
- tokens: bfloat16 [8192, 3584], P('seg'), may hold values from -6 to 6
- memory: bfloat16 [64, 3584], replicated, may hold values from -6 to 6
- norm_gain: float32 [3584], replicated, may hold values from 0.5 to 2
- post_gain: float32 [3584], replicated, may hold values from 0.5 to 2
- query_weight: bfloat16 [3584, 2048], P('seg'), may hold values from -0.09375 to 0.09375
- key_matrix: bfloat16 [3584, 1024], replicated, may hold values from -0.09375 to 0.09375
- value_matrix: bfloat16 [3584, 1024], replicated, may hold values from -0.09375 to 0.09375
- output_weight: bfloat16 [2048, 3584], P('seg'), may hold values from -0.125 to 0.125
- segment_weight: float32 [32], P('seg'), may hold values from 0.1 to 4
Outputs:
- token_out: bfloat16 [8192, 3584], P('seg')
- memory_out: bfloat16 [2048, 3584], P('seg')
- changes: float32 [3], replicated
The draws below stay inside these ranges and needn't reach their ends.
All inputs are finite; a program needn't handle non-finite values.
Results may differ from the reference program's by a relative error of at most 0.014.
Values may be sent and summed in bfloat16 or wider, within the bound.
A program may use at most 192 MiB of HBM per device.

```python
import math
import jax
import jax.numpy as jnp
from jax import lax

MODEL_WIDTH = 3584
HEAD_WIDTH = 256
HQ = 8
KEY_VALUE_HEADS = 4
MEM = 64
ITERS = 3
TOK_DEV = 256
SEGMENTS = 32
N_SEG = 32


def draw_segment_weight(key, part):
    ramp = jnp.arange(SEGMENTS).astype(jnp.float32) / max(SEGMENTS - 1, 1)
    level = jax.random.uniform(key, (SEGMENTS,), jnp.float32, 0.0, 1.0)
    return 0.1 + 0.3 * ramp + 3.6 * jnp.power(level, 8.0)


def level_of(stream_key, dims, split, low, high):
    factor_of = 1.0
    for dim, blocks in split:
        draws = jax.random.uniform(jax.random.fold_in(jax.random.fold_in(stream_key, 6), dim), (blocks,), jnp.float32, low / len(split), high / len(split))
        factor_of = factor_of * jnp.repeat(jnp.exp(draws), dims[dim] // blocks).reshape((-1,) + (1,) * (len(dims) - 1 - dim))
    return factor_of


def bell_draw(key, shape, spread, limit, shards=(), dtype=jnp.bfloat16):
    result = jax.random.normal(key, shape, jnp.float32) * spread
    if len(shards) > 0:
        result = level_of(key, shape, shards, -0.22, 0.18) * result
    return jnp.clip(result, min=-limit, max=limit).astype(dtype)


def setup_inputs(seed: int = 0) -> dict:
    key_list = jax.random.split(jax.random.key(seed), 10)
    return {
        "tokens": bell_draw(key_list[0], (SEGMENTS * TOK_DEV, MODEL_WIDTH), 1.0, 6.0, ((0, 32),)),
        "memory": bell_draw(key_list[1], (MEM, MODEL_WIDTH), 1.0, 6.0),
        "norm_gain": jnp.clip(jnp.exp(jax.random.uniform(key_list[2], (MODEL_WIDTH,), jnp.float32, math.log(0.5), math.log(2.0))), 0.5, 2.0),
        "post_gain": jnp.clip(jnp.exp(jax.random.uniform(key_list[3], (MODEL_WIDTH,), jnp.float32, math.log(0.5), math.log(2.0))), 0.5, 2.0),
        "query_weight": bell_draw(key_list[4], (MODEL_WIDTH, HQ * HEAD_WIDTH), MODEL_WIDTH ** -0.5, 0.09375, ((0, 32),)),
        "key_matrix": bell_draw(key_list[5], (MODEL_WIDTH, KEY_VALUE_HEADS * HEAD_WIDTH), MODEL_WIDTH ** -0.5, 0.09375),
        "value_matrix": bell_draw(key_list[6], (MODEL_WIDTH, KEY_VALUE_HEADS * HEAD_WIDTH), MODEL_WIDTH ** -0.5, 0.09375),
        "output_weight": bell_draw(key_list[7], (HQ * HEAD_WIDTH, MODEL_WIDTH), (HQ * HEAD_WIDTH) ** -0.5, 0.125, ((0, 32),)),
        "segment_weight": draw_segment_weight(jax.random.fold_in(key_list[9], 71), 0),
    }


eps = 1e-06

def prenorm(rows, gain):
    rows = rows.astype(jnp.float32)
    mean_sq = lax.optimization_barrier(jnp.mean(rows * rows, axis=-1, keepdims=True))
    return (rows / jnp.sqrt(mean_sq + eps) * gain).astype(jnp.bfloat16)

def attend(query_vectors, key_vectors, value_vectors, allowed):
    element_count = query_vectors.shape[0]
    feature_width = key_vectors.shape[0]
    query_heads_split = query_vectors.reshape(element_count, KEY_VALUE_HEADS, 2, HEAD_WIDTH).astype(jnp.float32)
    key_heads_split = key_vectors.reshape(feature_width, KEY_VALUE_HEADS, HEAD_WIDTH).astype(jnp.float32)
    value_heads_split = value_vectors.reshape(feature_width, KEY_VALUE_HEADS, HEAD_WIDTH).astype(jnp.float32)
    score = jnp.einsum('rgjd,kgd->gjrk', query_heads_split, key_heads_split)
    expo = jnp.where(allowed[None, None], jnp.exp(score), 0.0)
    denom = lax.optimization_barrier(jnp.sum(expo, axis=-1))
    weights = expo.astype(jnp.bfloat16).astype(jnp.float32)
    numer = jnp.einsum('gjrk,kgd->rgjd', weights, value_heads_split)
    denom = jnp.transpose(denom, (2, 0, 1))
    attn = numer / denom[:, :, :, None]
    return attn.reshape(element_count, HQ * HEAD_WIDTH).astype(jnp.bfloat16)

def finish(inputs, attn, output_weight, post_gain):
    proj = jnp.dot(attn, output_weight, preferred_element_type=jnp.float32)
    mean_sq = lax.optimization_barrier(jnp.mean(proj * proj, axis=-1, keepdims=True))
    return (inputs.astype(jnp.float32) + proj / jnp.sqrt(mean_sq + eps) * post_gain).astype(jnp.bfloat16)

def project(normed, weight):
    return jnp.dot(normed, weight, preferred_element_type=jnp.float32)

def reference(tokens, memory, norm_gain, post_gain, query_weight, key_matrix, value_matrix, output_weight, segment_weight):
    segs = N_SEG
    scale = 1.0 / HEAD_WIDTH ** 0.5
    seg_tokens = tokens.reshape(segs, TOK_DEV, MODEL_WIDTH)
    write_norm = prenorm(memory, norm_gain)
    write_q = (project(write_norm, query_weight) * scale).astype(jnp.bfloat16)
    write_k = project(write_norm, key_matrix).astype(jnp.bfloat16)
    write_v = project(write_norm, value_matrix).astype(jnp.bfloat16)

    def token_keys(rows):
        normed = prenorm(rows, norm_gain)
        return (project(normed, key_matrix).astype(jnp.bfloat16), project(normed, value_matrix).astype(jnp.bfloat16))
    tok_k, tok_v = lax.map(token_keys, seg_tokens)
    write_mask = jnp.concatenate([jnp.ones((MEM, MEM + TOK_DEV), bool), jnp.tril(jnp.ones((MEM, MEM), bool))], axis=1)

    def write_pass(items):
        read, keys_t, values_t = items
        normed = prenorm(read, norm_gain)
        read_k = project(normed, key_matrix).astype(jnp.bfloat16)
        read_v = project(normed, value_matrix).astype(jnp.bfloat16)
        key_vectors = jnp.concatenate([read_k, keys_t, write_k], axis=0)
        value_vectors = jnp.concatenate([read_v, values_t, write_v], axis=0)
        attn = attend(write_q, key_vectors, value_vectors, write_mask)
        return finish(memory, attn, output_weight, post_gain)
    read_all = jnp.broadcast_to(memory[None], (segs, MEM, MODEL_WIDTH))
    previous = read_all
    changes = []
    newest = previous
    read_used = read_all
    for step in range(ITERS):
        read_used = read_all
        newest = lax.map(write_pass, (read_all, tok_k, tok_v))
        diff = newest.astype(jnp.float32) - previous.astype(jnp.float32)
        per_segment = lax.optimization_barrier(jnp.sum(diff * diff, axis=(1, 2))) * segment_weight
        changes.append(jnp.sqrt(jnp.sum(per_segment) / (segs * MEM * MODEL_WIDTH) + eps))
        previous = newest
        read_all = jnp.concatenate([memory[None], newest[:-1]], axis=0)
    token_mask = jnp.concatenate([jnp.ones((TOK_DEV, MEM), bool), jnp.tril(jnp.ones((TOK_DEV, TOK_DEV), bool))], axis=1)

    def token_pass(items):
        rows, read, keys_t, values_t = items
        normed = prenorm(rows, norm_gain)
        query_vectors = (project(normed, query_weight) * scale).astype(jnp.bfloat16)
        read_norm = prenorm(read, norm_gain)
        read_k = project(read_norm, key_matrix).astype(jnp.bfloat16)
        read_v = project(read_norm, value_matrix).astype(jnp.bfloat16)
        key_vectors = jnp.concatenate([read_k, keys_t], axis=0)
        value_vectors = jnp.concatenate([read_v, values_t], axis=0)
        attn = attend(query_vectors, key_vectors, value_vectors, token_mask)
        return finish(rows, attn, output_weight, post_gain)
    token_out = lax.map(token_pass, (seg_tokens, read_used, tok_k, tok_v))
    return (token_out.reshape(segs * TOK_DEV, MODEL_WIDTH), newest.reshape(segs * MEM, MODEL_WIDTH), jnp.stack(changes).astype(jnp.float32))
```

```python
import functools

import jax
import jax.numpy as jnp
from jax import lax
from jax.experimental import pallas as pl
from jax.experimental.pallas import tpu as pltpu
from jax.sharding import PartitionSpec as P


HEAD_WIDTH = 256
KEY_VALUE_HEADS = 4
ITERS = 3
LANES = 128
MESH = pl.DeviceIdType.MESH


eps = 1e-06


def from_behind(block, axis, distance):
    devices = range(lax.axis_size(axis))
    route = [(i - distance, i) for i in devices if i - distance in devices]
    return lax.ppermute(block, axis, route)


def prenorm(rows, gain):
    rows = rows.astype(jnp.float32)
    mean_sq = jnp.mean(rows * rows, axis=-1, keepdims=True)
    return (rows / jnp.sqrt(mean_sq + eps) * gain).astype(jnp.bfloat16)


def reduce_kernel(n, scale, part_ref, out_ref, held, total, final, send1, recv1, send2, recv2):
    me = lax.axis_index("seg") // 2
    core = lax.rem(lax.axis_index("seg"), 2)

    def scatter(k):
        to = lax.rem(me + k, n)
        return pltpu.make_async_remote_copy(
            src_ref=part_ref.at[to],
            dst_ref=held.at[k],
            send_sem=send1.at[k],
            recv_sem=recv1.at[k],
            device_id=(2 * to + core,),
            device_id_type=MESH,
        )

    def spread(k):
        to = lax.rem(me + k, n)
        return pltpu.make_async_remote_copy(
            src_ref=final,
            dst_ref=out_ref.at[me],
            send_sem=send2.at[k],
            recv_sem=recv2.at[k],
            device_id=(2 * to + core,),
            device_id_type=MESH,
        )

    @pl.loop(1, n)
    def _(k):
        scatter(k).start()

    total[...] = part_ref[me]

    @pl.loop(1, n)
    def _(k):
        scatter(k).wait_recv()
        total[...] += held[k]

    final[...] = (total[...] * scale).astype(final.dtype)

    @pl.loop(1, n)
    def _(k):
        spread(k).start()

    out_ref[me] = final[...]

    @pl.loop(1, n)
    def _(k):
        scatter(k).wait_send()
        spread(k).wait()


def all_sum(parts, scale):
    n = parts.shape[0]
    sems = pltpu.SemaphoreType.DMA((n,))
    return pl.pallas_call(
        functools.partial(reduce_kernel, n, scale),
        out_shape=jax.ShapeDtypeStruct(parts.shape, jnp.bfloat16),
        in_specs=[pl.BlockSpec(memory_space=pltpu.VMEM)],
        out_specs=pl.BlockSpec(memory_space=pltpu.VMEM),
        scratch_shapes=[
            pltpu.VMEM(parts.shape, parts.dtype),
            pltpu.VMEM(parts.shape[1:], parts.dtype),
            pltpu.VMEM(parts.shape[1:], jnp.bfloat16),
            sems,
            sems,
            sems,
            sems,
        ],
        compiler_params=pltpu.CompilerParams(has_side_effects=True),
        cost_estimate=pl.CostEstimate(flops=0, bytes_accessed=30_000_000, transcendentals=0),
        name="query_sum",
    )(parts)


def total_kernel(n, part_ref, out_ref, held, send, recv):
    me = lax.axis_index("seg")

    def copy(k):
        return pltpu.make_async_remote_copy(
            src_ref=part_ref,
            dst_ref=held.at[me],
            send_sem=send.at[k],
            recv_sem=recv.at[k],
            device_id=(lax.rem(me + k, n),),
            device_id_type=MESH,
        )

    @pl.loop(1, n)
    def _(k):
        copy(k).start()

    held[me] = part_ref[...]

    @pl.loop(1, n)
    def _(k):
        copy(k).wait()

    out_ref[...] = jnp.sum(held[...], axis=0)


def small_sum(part, n):
    sems = pltpu.SemaphoreType.DMA((n,))
    return pl.pallas_call(
        functools.partial(total_kernel, n),
        out_shape=jax.ShapeDtypeStruct(part.shape, part.dtype),
        in_specs=[pl.BlockSpec(memory_space=pltpu.VMEM)],
        out_specs=pl.BlockSpec(memory_space=pltpu.VMEM),
        scratch_shapes=[pltpu.VMEM((n,) + part.shape, part.dtype), sems, sems],
        compiler_params=pltpu.CompilerParams(has_side_effects=True),
        cost_estimate=pl.CostEstimate(flops=0, bytes_accessed=8_000_000, transcendentals=0),
        name="change_sum",
    )(part)


def attend_kernel(first, keys, q_ref, rk_ref, rv_ref, k_ref, v_ref, out_ref):
    rows = q_ref.shape[0]
    nt = (((1,), (1,)), ((), ()))
    row = lax.broadcasted_iota(jnp.int32, (rows, keys), 0)
    col = lax.broadcasted_iota(jnp.int32, (rows, keys), 1)
    allowed = col <= row + first
    for half in range(2):
        cols = slice(half * HEAD_WIDTH, (half + 1) * HEAD_WIDTH)
        q = q_ref[:, cols]
        own = lax.dot_general(q, k_ref[:keys], nt, preferred_element_type=jnp.float32)
        own = jnp.where(allowed, jnp.exp(own), 0.0)
        read = jnp.exp(
            lax.dot_general(q, rk_ref[...], nt, preferred_element_type=jnp.float32)
        )
        denom = jnp.sum(own, axis=-1, keepdims=True) + jnp.sum(read, axis=-1, keepdims=True)
        numer = jnp.dot(
            own.astype(jnp.bfloat16), v_ref[:keys], preferred_element_type=jnp.float32
        ) + jnp.dot(read.astype(jnp.bfloat16), rv_ref[...], preferred_element_type=jnp.float32)
        out_ref[:, cols] = (numer / denom).astype(jnp.bfloat16)


def attend(q, read_k, read_v, local_k, local_v, first, keys):
    rows, width = q.shape
    mem, total = read_k.shape[0], local_k.shape[0]
    at = lambda h: (0, h)
    return pl.pallas_call(
        functools.partial(attend_kernel, first, keys),
        grid=(KEY_VALUE_HEADS,),
        out_shape=jax.ShapeDtypeStruct((rows, width), jnp.bfloat16),
        in_specs=[
            pl.BlockSpec((rows, 2 * HEAD_WIDTH), at),
            pl.BlockSpec((mem, HEAD_WIDTH), at),
            pl.BlockSpec((mem, HEAD_WIDTH), at),
            pl.BlockSpec((total, HEAD_WIDTH), at),
            pl.BlockSpec((total, HEAD_WIDTH), at),
        ],
        out_specs=pl.BlockSpec((rows, 2 * HEAD_WIDTH), at),
        cost_estimate=pl.CostEstimate(
            flops=4 * rows * width * (keys + mem), bytes_accessed=6_000_000, transcendentals=0
        ),
        name="attend",
    )(q, read_k, read_v, local_k, local_v)


def finish(inputs, attn, output_weight, post_gain):
    proj = jnp.dot(attn, output_weight, preferred_element_type=jnp.float32)
    mean_sq = jnp.mean(proj * proj, axis=-1, keepdims=True)
    return (inputs.astype(jnp.float32) + proj / jnp.sqrt(mean_sq + eps) * post_gain).astype(
        jnp.bfloat16
    )


def shards(
    tokens,
    memory,
    norm_gain,
    post_gain,
    query_weight,
    key_matrix,
    value_matrix,
    output_weight,
    segment_weight,
):
    n = lax.axis_size("seg")
    me = lax.axis_index("seg")
    tok_rows = tokens.shape[0]
    mem_rows, feature_width = memory.shape
    own_rows, query_width = query_weight.shape
    scale = 1.0 / HEAD_WIDTH**0.5
    output_full = lax.all_gather(output_weight, "seg", axis=0, tiled=True)

    mem_norm = prenorm(memory, norm_gain)
    own_cols = lax.dynamic_slice_in_dim(mem_norm, me * own_rows, own_rows, axis=1)
    part = jnp.dot(own_cols, query_weight, preferred_element_type=jnp.float32)
    blocks = query_width // LANES
    part = jnp.transpose(part.reshape(mem_rows, blocks, LANES), (1, 0, 2))
    core = lax.rem(me, 2)
    pairs = [(i, i + 1 - 2 * (i % 2)) for i in range(n)]
    share = blocks // 2
    kept = lax.dynamic_slice_in_dim(part, core * share, share, axis=0)
    given = lax.dynamic_slice_in_dim(part, (1 - core) * share, share, axis=0)
    kept = kept + lax.ppermute(given, "seg", pairs)
    peers = n // 2
    own_q = all_sum(kept.reshape(peers, mem_rows * share // peers, LANES), scale)
    own_q = own_q.reshape(share, mem_rows, LANES)
    other_q = lax.ppermute(own_q, "seg", pairs)
    low = core == 0
    write_q = jnp.concatenate(
        [jnp.where(low, own_q, other_q), jnp.where(low, other_q, own_q)], axis=0
    )
    write_q = jnp.transpose(write_q, (1, 0, 2)).reshape(mem_rows, query_width)

    own_query, write_q = lax.optimization_barrier((query_weight, write_q))
    query_full = lax.all_gather(own_query, "seg", axis=0, tiled=True)

    normed = prenorm(jnp.concatenate([tokens, memory], axis=0), norm_gain)
    local_k = jnp.dot(normed, key_matrix, preferred_element_type=jnp.float32).astype(jnp.bfloat16)
    local_v = jnp.dot(normed, value_matrix, preferred_element_type=jnp.float32).astype(jnp.bfloat16)
    total_rows = tok_rows + mem_rows
    first = jnp.int32(0) == me
    previous = memory
    squares = []
    own_weight = segment_weight[0]
    count_all = n * mem_rows * feature_width
    read_k, read_v = local_k[tok_rows:], local_v[tok_rows:]
    for step in range(ITERS):
        attn = attend(write_q, read_k, read_v, local_k, local_v, tok_rows, total_rows)
        newest = finish(memory, attn, output_full, post_gain)
        diff = newest.astype(jnp.float32) - previous.astype(jnp.float32)
        squares.append(jnp.sum(diff * diff) * own_weight)
        previous = newest
        if step + 1 < ITERS:
            read = jnp.where(first, memory, from_behind(newest, "seg", 1))
            read_norm = prenorm(read, norm_gain)
            read_k = jnp.dot(read_norm, key_matrix, preferred_element_type=jnp.float32).astype(
                jnp.bfloat16
            )
            read_v = jnp.dot(read_norm, value_matrix, preferred_element_type=jnp.float32).astype(
                jnp.bfloat16
            )
    squares = jnp.broadcast_to(jnp.pad(jnp.stack(squares), (0, LANES - ITERS))[None], (8, LANES))
    totals = small_sum(squares, n)[0, :ITERS]
    change_vec = jnp.sqrt(totals / count_all + eps)

    query_acc = jnp.dot(normed[:tok_rows], query_full, preferred_element_type=jnp.float32)
    query_vectors = (query_acc * scale).astype(jnp.bfloat16)
    attn = attend(query_vectors, read_k, read_v, local_k, local_v, 0, tok_rows)
    token_out = finish(tokens, attn, output_full, post_gain)
    return (token_out, previous, change_vec)


def chip_grid(chips):
    side = 1
    while (2 * side) ** 3 <= chips and chips % (4 * side * side) == 0:
        side *= 2
    return chips // (side * side), side


def fits(tokens, memory, norm_gain, post_gain, query_weight, *rest):
    n = lax.axis_size("seg")
    own_rows, query_width = query_weight.shape
    out_rows = rest[2].shape[0]
    mem_rows = memory.shape[0]
    if n % 2 or n < 8:
        return False
    _, side = chip_grid(n // 2)
    plane = 2 * side * side
    piece = mem_rows * (query_width // LANES) // n
    return (
        side == 2
        and own_rows % 16 == 0
        and out_rows % 16 == 0
        and (own_rows * plane) % LANES == 0
        and piece % 16 == 0
        and mem_rows % piece == 0
        and memory.shape[1] >= 256
        and own_rows + LANES <= 256
    )


def nearest(position, k, size):
    value = 0
    for p in range(size):
        order = sorted(range(size), key=lambda q: (abs(q - p), q))
        value = jnp.where(position == p, order[k], value)
    return value


def arrival_order(depth, side):
    sheet = sorted(
        [(k, j) for k in range(depth) for j in range(side)],
        key=lambda e: (e[0] + e[1], e[1] == 0, e[0]),
    )
    items, clock = [], 0
    for k, j in sheet:
        if k + j:
            items.append((k + j, 0, (k, j, 0)))
        clock = max(clock, k + j) + 1
        for i in range(1, side):
            items.append((clock + i - 1, 1, (k, j, i)))
    return [e for _, _, e in sorted(items)]


def fused_kernel(
    n,
    tokens_hbm,
    memory_hbm,
    norm_gain,
    post_gain,
    wq_hbm,
    wk_hbm,
    wv_hbm,
    wo_hbm,
    seg_weight,
    token_out,
    memory_out,
    change_out,
    tokens,
    memory,
    wk,
    wv,
    wq,
    wo,
    window,
    normed,
    part,
    swapped,
    kept,
    held,
    piece_out,
    pieces,
    write_q,
    local_k,
    local_v,
    sent_kv,
    read_kv,
    attn,
    proj,
    previous,
    newnorm,
    query,
    change,
    changes,
    load_sem,
    gather_send,
    gather_recv,
    pair_recv,
    swap_sem,
    sum_send,
    sum_recv,
    spread_send,
    spread_recv,
    kv_send,
    kv_recv,
    change_send,
    change_recv,
    store_sem,
):
    me = lax.axis_index("seg")
    core = lax.rem(me, 2)
    partner = me + 1 - 2 * core
    chip = me // 2
    chips = n // 2
    depth, side = chip_grid(chips)
    tok_rows, width = tokens.shape
    mem_rows = memory.shape[0]
    all_rows = tok_rows + mem_rows
    fast, mid, slow = (
        lax.rem(chip, side),
        lax.rem(chip // side, side),
        chip // (side * side),
    )
    scale = 1.0 / HEAD_WIDTH**0.5
    f32, bf16 = jnp.float32, jnp.bfloat16
    u = mid * (1 - core) + fast * core
    v = fast * (1 - core) + mid * core
    u_step = side * (1 - core) + core
    v_step = (1 - core) + side * core
    z_step = side * side
    full = (wo, wq)
    block_rows = (wo_hbm.shape[0], wq_hbm.shape[0])
    query_width = wq.shape[1]

    def hint(x, m):
        return pl.multiple_of(x, m)

    def block_at(w, device):
        rows = block_rows[w]
        return full[w].at[pl.ds(hint(device * rows, 16), rows)]

    def remote(src, dst, send, recv, device):
        return pltpu.make_async_remote_copy(
            src_ref=src,
            dst_ref=dst,
            send_sem=send,
            recv_sem=recv,
            device_id=(device,),
            device_id_type=MESH,
        )

    def place(k, j, i):
        z = nearest(slow, k, depth)
        uu = u if j == 0 else 1 - u
        vv = v if i == 0 else 1 - v
        return z, z * z_step + uu * u_step + vv * v_step

    def rank(k, j, i):
        return (k * side + j) * side + i

    def moves(w, k, j, i):
        z, origin = place(k, j, i)
        block = block_at(w, 2 * origin + core)
        ports = 5

        def copy(port, device, recv):
            return remote(
                block,
                block,
                gather_send.at[w, rank(k, j, i) * ports + port],
                recv.at[w, origin],
                device,
            )

        found = []
        if j == 0 and i == 0:
            up = slow + 1 < depth
            down = slow > 0
            if k:
                up = jnp.logical_and(up, z < slow)
                down = jnp.logical_and(down, z > slow)
            found.append((up, copy(0, me + 2 * z_step, gather_recv)))
            found.append((down, copy(1, me - 2 * z_step, gather_recv)))
        if i == 0 and j == 0:
            found.append((None, copy(2, me + 2 * u_step * (1 - 2 * u), gather_recv)))
        if i == 0:
            found.append((None, copy(3, me + 2 * v_step * (1 - 2 * v), gather_recv)))
        found.append((None, copy(4, partner, pair_recv)))
        return found

    def start(items):
        for guard, copy in items:
            if guard is None:
                copy.start()
            else:
                pl.when(guard)(copy.start)

    def arrive(w, k, j, i):
        _, origin = place(k, j, i)
        block = block_at(w, 2 * origin + core)
        remote(
            block, block, gather_send.at[w, 0], gather_recv.at[w, origin], partner
        ).wait_recv()

    def arrived(w, e):
        arrive(w, *e)
        start(moves(w, *e))

    def pair_arrive(w, k, j, i):
        _, origin = place(k, j, i)
        block = block_at(w, 2 * origin + 1 - core)
        remote(
            block, block, gather_send.at[w, 0], pair_recv.at[w, origin], partner
        ).wait_recv()

    events = arrival_order(depth, side)
    everything = [(0, 0, 0)] + events

    def load(src, dst, i):
        return pltpu.make_async_copy(src, dst, load_sem.at[i])

    off = me * block_rows[1]
    first_lane = jnp.minimum(off // LANES * LANES, width - 256)
    shift = off - first_lane
    loads = [
        load(wo_hbm, block_at(0, me), 0),
        load(memory_hbm, memory, 1),
        load(wq_hbm, block_at(1, me), 2),
        load(tokens_hbm, tokens, 3),
        load(wk_hbm, wk, 4),
        load(wv_hbm, wv, 5),
    ]
    for copy in loads:
        copy.start()
    window[...] = jnp.zeros_like(window)
    own_window = load(
        wq_hbm, window.at[pl.ds(hint(shift, 16), block_rows[1])], 6
    )
    own_window.start()

    def norm_rows(src, dst, at, rows):
        step_rows = 16

        @pl.loop(0, rows // step_rows)
        def _(t):
            here = pl.ds(hint(t * step_rows, step_rows), step_rows)
            x = src[here, :].astype(f32)
            mean_sq = jnp.sum(x * x, axis=-1, keepdims=True) / width
            there = pl.ds(hint(at + t * step_rows, step_rows), step_rows)
            dst[there, :] = (x / jnp.sqrt(mean_sq + eps) * norm_gain[...]).astype(bf16)

    def times(lhs, weight, dst, tile):
        @pl.loop(0, weight.shape[1] // tile)
        def _(t):
            cols = pl.ds(hint(t * tile, tile), tile)
            dst[:, cols] = jnp.dot(
                lhs[...], weight[:, cols], preferred_element_type=f32
            ).astype(dst.dtype)

    nt = (((1,), (1,)), ((), ()))

    def attend_rows(q_ref, rows, rk, rv, first, keys, pre):
        row = lax.broadcasted_iota(jnp.int32, (rows, keys), 0)
        col = lax.broadcasted_iota(jnp.int32, (rows, keys), 1)
        allowed = col <= row + first

        @pl.loop(0, KEY_VALUE_HEADS)
        def _(g):
            kv_cols = pl.ds(hint(g * HEAD_WIDTH, HEAD_WIDTH), HEAD_WIDTH)
            kk = local_k[0:keys, kv_cols]
            vv = local_v[0:keys, kv_cols]
            rkk = rk[:, kv_cols]
            rvv = rv[:, kv_cols]
            for half in range(2):
                cols = pl.ds(hint((2 * g + half) * HEAD_WIDTH, HEAD_WIDTH), HEAD_WIDTH)
                q = q_ref[0:rows, cols]
                if pre:
                    q = (q * scale).astype(bf16)
                own = lax.dot_general(q, kk, nt, preferred_element_type=f32)
                own = jnp.where(allowed, jnp.exp(own), 0.0)
                read = jnp.exp(lax.dot_general(q, rkk, nt, preferred_element_type=f32))
                denom = jnp.sum(own, axis=-1, keepdims=True) + jnp.sum(
                    read, axis=-1, keepdims=True
                )
                numer = jnp.dot(
                    own.astype(bf16), vv, preferred_element_type=f32
                ) + jnp.dot(read.astype(bf16), rvv, preferred_element_type=f32)
                attn[0:rows, cols] = (numer / denom).astype(bf16)

    def project(rows):
        tile = 512

        @pl.loop(0, width // tile)
        def _(t):
            cols = pl.ds(hint(t * tile, tile), tile)
            proj[0:rows, cols] = jnp.dot(
                attn[0:rows, :], wo[:, cols], preferred_element_type=f32
            )

    def layer_rows(src, here):
        p = proj[here, :]
        mean_sq = jnp.sum(p * p, axis=-1, keepdims=True) / width
        x = src[here, :].astype(f32)
        return (x + p / jnp.sqrt(mean_sq + eps) * post_gain[...]).astype(bf16)

    def write_rows(step):
        before = memory if step == 0 else previous
        change[...] = jnp.zeros_like(change) if step == 0 else change[...]
        lane = lax.broadcasted_iota(jnp.int32, change.shape, 1)

        @pl.loop(0, mem_rows // 16)
        def _(t):
            here = pl.ds(hint(t * 16, 16), 16)
            out = layer_rows(memory, here)
            o = out.astype(f32)
            diff = o - before[here, :].astype(f32)
            total = jnp.sum(diff * diff, keepdims=True)
            change[...] += jnp.where(lane == step, total * seg_weight[0], 0.0)
            previous[here, :] = out
            if step + 1 < ITERS:
                mean_sq = jnp.sum(o * o, axis=-1, keepdims=True) / width
                newnorm[here, :] = (o / jnp.sqrt(mean_sq + eps) * norm_gain[...]).astype(bf16)

    right = lax.rem(me + 1, n)

    def kv_copy(step, which):
        return remote(
            sent_kv.at[step, which],
            read_kv.at[step, which],
            kv_send.at[step, which],
            kv_recv.at[step, which],
            right,
        )

    def send_kv(step):
        for which, weight in enumerate((wk, wv)):
            times(newnorm, weight, sent_kv.at[step, which], 512)
            pl.when(me + 1 < n)(kv_copy(step, which).start)

    def wait_kv(step):
        @pl.when(me > 0)
        def _():
            for which in range(2):
                kv_copy(step, which).wait_recv()

        @pl.when(me == 0)
        def _():
            for which, local in enumerate((local_k, local_v)):
                read_kv[step, which] = local[tok_rows:all_rows, :]

    loads[0].wait()
    start(moves(0, 0, 0, 0))
    loads[1].wait()
    norm_rows(memory, normed, tok_rows, mem_rows)
    own_window.wait()
    piece = pieces.shape[1]
    per_block = mem_rows // piece
    half_width = query_width // 2
    own_cols = normed[tok_rows:all_rows, pl.ds(hint(first_lane, LANES), 256)]
    for c in range(2):
        rows_of = jnp.dot(
            own_cols,
            window[:, c * half_width : (c + 1) * half_width],
            preferred_element_type=f32,
        )
        for t in range(chips):
            at = t // per_block * LANES
            down = t % per_block * piece
            part[c, t] = rows_of[down : down + piece, at : at + LANES]
    swap = remote(part.at[1 - core], swapped, swap_sem.at[0], swap_sem.at[1], partner)
    swap.start()
    loads[3].wait()
    norm_rows(tokens, normed, 0, tok_rows)
    swap.wait_recv()
    kept[...] = part[core] + swapped[...]

    def scatter(k):
        to = lax.rem(chip + k, chips)
        return remote(
            kept.at[to], held.at[k], sum_send.at[k], sum_recv.at[k], 2 * to + core
        )

    @pl.loop(1, chips)
    def _(k):
        scatter(k).start()

    loads[4].wait()
    times(normed, wk, local_k, 512)
    early = [e for e in events if sum(e) == 1]
    late = [e for e in events if sum(e) > 1]
    for e in early:
        arrived(0, e)

    @pl.loop(1, chips)
    def _(k):
        scatter(k).wait_recv()

    piece_sum = kept[chip]
    for k in range(1, chips):
        piece_sum += held[k]
    piece_out[...] = (piece_sum * scale).astype(bf16)

    def spread(k):
        to = lax.rem(me + k, n)
        return remote(
            piece_out, pieces.at[me], spread_send.at[k], spread_recv.at[k], to
        )

    @pl.loop(1, n)
    def _(k):
        spread(k).start()

    pieces[me] = piece_out[...]
    loads[5].wait()
    times(normed, wv, local_v, 512)

    first_q = [e for e in events if e[1] == 0 and e[2] == 0]
    rest_q = [e for e in events if e[1] or e[2]]
    middle = len(late) // 2
    for e in late[:middle]:
        arrived(0, e)

    @pl.loop(1, n)
    def _(k):
        spread(k).wait_recv()

    for d in range(n):
        t, c = d // 2, d % 2
        at = c * half_width + t // per_block * LANES
        down = t % per_block * piece
        write_q[down : down + piece, at : at + LANES] = pieces[d]
    attend_rows(
        write_q,
        mem_rows,
        local_k.at[pl.ds(tok_rows, mem_rows)],
        local_v.at[pl.ds(tok_rows, mem_rows)],
        tok_rows,
        all_rows,
        False,
    )
    tail = list(late[middle:])
    forwards = [e for e in tail if e[2] == 0]
    passed = tail.index(forwards[-1]) + 1 if forwards else 0
    for e in tail[:passed]:
        arrived(0, e)
    loads[2].wait()
    start(moves(1, 0, 0, 0))
    queue = list(first_q)
    for e in tail[passed:]:
        arrived(0, e)
        if queue:
            arrived(1, queue.pop(0))
    for e in queue:
        arrived(1, e)
    for e in everything:
        pair_arrive(0, *e)

    ahead = list(rest_q)

    def take(count):
        for _ in range(min(count, len(ahead))):
            arrived(1, ahead.pop(0))

    project(mem_rows)
    write_rows(0)
    send_kv(0)
    take(2)
    wait_kv(0)
    for step in range(1, ITERS):
        rk, rv = read_kv.at[step - 1, 0], read_kv.at[step - 1, 1]
        attend_rows(write_q, mem_rows, rk, rv, tok_rows, all_rows, False)
        project(mem_rows)
        write_rows(step)
        if step + 1 < ITERS:
            send_kv(step)
            take(2)
            wait_kv(step)
            take(2)
    store = pltpu.make_async_copy(previous, memory_out, store_sem.at[0])
    store.start()

    def share(k):
        to = lax.rem(me + k, n)
        return remote(change, changes.at[me], change_send.at[k], change_recv.at[k], to)

    @pl.loop(1, n)
    def _(k):
        share(k).start()

    changes[me] = change[...]

    plane_rows = block_rows[1] * 2 * side * side

    def query_plane(k):
        z = nearest(slow, k, depth)
        at = hint(z * plane_rows, LANES)
        tile = 512

        @pl.loop(0, query_width // tile)
        def _(t):
            cols = pl.ds(hint(t * tile, tile), tile)
            more = jnp.dot(
                normed[0:tok_rows, pl.ds(at, plane_rows)],
                wq[pl.ds(at, plane_rows), cols],
                preferred_element_type=f32,
            )
            if k == 0:
                query[:, cols] = more
            else:
                query[:, cols] += more

    for k in range(depth):
        while any(e[0] == k for e in ahead):
            take(1)
        for e in everything:
            if e[0] == k:
                pair_arrive(1, *e)
        query_plane(k)
    rk, rv = read_kv.at[ITERS - 2, 0], read_kv.at[ITERS - 2, 1]
    attend_rows(query, tok_rows, rk, rv, 0, tok_rows, True)
    project(tok_rows)

    @pl.loop(0, tok_rows // 16)
    def _(t):
        here = pl.ds(hint(t * 16, 16), 16)
        tokens[here, :] = layer_rows(tokens, here)

    store_tokens = pltpu.make_async_copy(tokens, token_out, store_sem.at[1])
    store_tokens.start()

    @pl.loop(1, n)
    def _(k):
        share(k).wait_recv()

    count_all = n * mem_rows * width
    total = changes[0]
    for d in range(1, n):
        total += changes[d]
    change_out[...] = jnp.sqrt(total / count_all + eps)

    swap.wait_send()
    for w in range(2):
        for e in everything:
            for guard, copy in moves(w, *e):
                if guard is None:
                    copy.wait_send()
                else:
                    pl.when(guard)(copy.wait_send)

    @pl.loop(1, chips)
    def _(k):
        scatter(k).wait_send()

    @pl.loop(1, n)
    def _(k):
        spread(k).wait_send()
        share(k).wait_send()

    @pl.when(me + 1 < n)
    def _():
        for step in range(ITERS - 1):
            for which in range(2):
                kv_copy(step, which).wait_send()

    store.wait()
    store_tokens.wait()


def fused(
    tokens,
    memory,
    norm_gain,
    post_gain,
    query_weight,
    key_matrix,
    value_matrix,
    output_weight,
    segment_weight,
):
    n = lax.axis_size("seg")
    chips = n // 2
    tok_rows, width = tokens.shape
    mem_rows = memory.shape[0]
    own_rows, query_width = query_weight.shape
    kv_width = key_matrix.shape[1]
    all_rows = tok_rows + mem_rows
    piece = mem_rows * (query_width // LANES) // n
    f32, bf16 = jnp.float32, jnp.bfloat16
    anywhere = pl.BlockSpec(memory_space=pl.ANY)
    in_vmem = pl.BlockSpec(memory_space=pltpu.VMEM)
    dma = pltpu.SemaphoreType.DMA
    outs = pl.pallas_call(
        functools.partial(fused_kernel, n),
        out_shape=(
            jax.ShapeDtypeStruct(tokens.shape, bf16),
            jax.ShapeDtypeStruct(memory.shape, bf16),
            jax.ShapeDtypeStruct((8, LANES), f32),
        ),
        in_specs=[
            anywhere,
            anywhere,
            in_vmem,
            in_vmem,
            anywhere,
            anywhere,
            anywhere,
            anywhere,
            pl.BlockSpec(memory_space=pltpu.SMEM),
        ],
        out_specs=(anywhere, anywhere, in_vmem),
        scratch_shapes=[
            pltpu.VMEM(tokens.shape, bf16),
            pltpu.VMEM(memory.shape, bf16),
            pltpu.VMEM(key_matrix.shape, bf16),
            pltpu.VMEM(value_matrix.shape, bf16),
            pltpu.VMEM((n * own_rows, query_width), bf16),
            pltpu.VMEM((query_width, width), bf16),
            pltpu.VMEM((256, query_width), bf16),
            pltpu.VMEM((all_rows, width), bf16),
            pltpu.VMEM((2, chips, piece, LANES), f32),
            pltpu.VMEM((chips, piece, LANES), f32),
            pltpu.VMEM((chips, piece, LANES), f32),
            pltpu.VMEM((chips, piece, LANES), f32),
            pltpu.VMEM((piece, LANES), bf16),
            pltpu.VMEM((n, piece, LANES), bf16),
            pltpu.VMEM((mem_rows, query_width), bf16),
            pltpu.VMEM((all_rows, kv_width), bf16),
            pltpu.VMEM((all_rows, kv_width), bf16),
            pltpu.VMEM((ITERS - 1, 2, mem_rows, kv_width), bf16),
            pltpu.VMEM((ITERS - 1, 2, mem_rows, kv_width), bf16),
            pltpu.VMEM((tok_rows, query_width), bf16),
            pltpu.VMEM((tok_rows, width), f32),
            pltpu.VMEM(memory.shape, bf16),
            pltpu.VMEM(memory.shape, bf16),
            pltpu.VMEM((tok_rows, query_width), f32),
            pltpu.VMEM((8, LANES), f32),
            pltpu.VMEM((n, 8, LANES), f32),
            dma((7,)),
            dma((2, chips * 5)),
            dma((2, chips)),
            dma((2, chips)),
            dma((2,)),
            dma((chips,)),
            dma((chips,)),
            dma((n,)),
            dma((n,)),
            dma((ITERS - 1, 2)),
            dma((ITERS - 1, 2)),
            dma((n,)),
            dma((n,)),
            dma((2,)),
        ],
        compiler_params=pltpu.CompilerParams(
            has_side_effects=True, vmem_limit_bytes=67_000_000
        ),
        name="segments",
    )(
        tokens,
        memory,
        norm_gain.reshape(1, width),
        post_gain.reshape(1, width),
        query_weight,
        key_matrix,
        value_matrix,
        output_weight,
        segment_weight,
    )
    return outs[0], outs[1], outs[2][0, :ITERS]


def solution(mesh):
    def step(*args):
        if fits(*args):
            return fused(*args)
        return shards(*args)

    in_specs = (
        P("seg", None),
        P(),
        P(),
        P(),
        P("seg", None),
        P(),
        P(),
        P("seg", None),
        P("seg"),
    )
    out_specs = (P("seg", None), P("seg", None), P())
    return jax.shard_map(
        step, mesh=mesh, in_specs=in_specs, out_specs=out_specs, check_vma=False
    )
```

```python
import functools

import jax
import jax.numpy as jnp
from jax import lax
from jax.experimental import pallas as pl
from jax.experimental.pallas import tpu as pltpu
from jax.sharding import PartitionSpec as P


HEAD_WIDTH = 256
KEY_VALUE_HEADS = 4
ITERS = 3
LANES = 128
MESH = pl.DeviceIdType.MESH


eps = 1e-06


def from_behind(block, axis, distance):
    devices = range(lax.axis_size(axis))
    route = [(i - distance, i) for i in devices if i - distance in devices]
    return lax.ppermute(block, axis, route)


def prenorm(rows, gain):
    rows = rows.astype(jnp.float32)
    mean_sq = jnp.mean(rows * rows, axis=-1, keepdims=True)
    return (rows / jnp.sqrt(mean_sq + eps) * gain).astype(jnp.bfloat16)


def reduce_kernel(n, scale, part_ref, out_ref, held, total, final, send1, recv1, send2, recv2):
    me = lax.axis_index("seg") // 2
    core = lax.rem(lax.axis_index("seg"), 2)

    def scatter(k):
        to = lax.rem(me + k, n)
        return pltpu.make_async_remote_copy(
            src_ref=part_ref.at[to],
            dst_ref=held.at[k],
            send_sem=send1.at[k],
            recv_sem=recv1.at[k],
            device_id=(2 * to + core,),
            device_id_type=MESH,
        )

    def spread(k):
        to = lax.rem(me + k, n)
        return pltpu.make_async_remote_copy(
            src_ref=final,
            dst_ref=out_ref.at[me],
            send_sem=send2.at[k],
            recv_sem=recv2.at[k],
            device_id=(2 * to + core,),
            device_id_type=MESH,
        )

    @pl.loop(1, n)
    def _(k):
        scatter(k).start()

    total[...] = part_ref[me]

    @pl.loop(1, n)
    def _(k):
        scatter(k).wait_recv()
        total[...] += held[k]

    final[...] = (total[...] * scale).astype(final.dtype)

    @pl.loop(1, n)
    def _(k):
        spread(k).start()

    out_ref[me] = final[...]

    @pl.loop(1, n)
    def _(k):
        scatter(k).wait_send()
        spread(k).wait()


def all_sum(parts, scale):
    n = parts.shape[0]
    sems = pltpu.SemaphoreType.DMA((n,))
    return pl.pallas_call(
        functools.partial(reduce_kernel, n, scale),
        out_shape=jax.ShapeDtypeStruct(parts.shape, jnp.bfloat16),
        in_specs=[pl.BlockSpec(memory_space=pltpu.VMEM)],
        out_specs=pl.BlockSpec(memory_space=pltpu.VMEM),
        scratch_shapes=[
            pltpu.VMEM(parts.shape, parts.dtype),
            pltpu.VMEM(parts.shape[1:], parts.dtype),
            pltpu.VMEM(parts.shape[1:], jnp.bfloat16),
            sems,
            sems,
            sems,
            sems,
        ],
        compiler_params=pltpu.CompilerParams(has_side_effects=True),
        cost_estimate=pl.CostEstimate(flops=0, bytes_accessed=30_000_000, transcendentals=0),
        name="query_sum",
    )(parts)


def total_kernel(n, part_ref, out_ref, held, send, recv):
    me = lax.axis_index("seg")

    def copy(k):
        return pltpu.make_async_remote_copy(
            src_ref=part_ref,
            dst_ref=held.at[me],
            send_sem=send.at[k],
            recv_sem=recv.at[k],
            device_id=(lax.rem(me + k, n),),
            device_id_type=MESH,
        )

    @pl.loop(1, n)
    def _(k):
        copy(k).start()

    held[me] = part_ref[...]

    @pl.loop(1, n)
    def _(k):
        copy(k).wait()

    out_ref[...] = jnp.sum(held[...], axis=0)


def small_sum(part, n):
    sems = pltpu.SemaphoreType.DMA((n,))
    return pl.pallas_call(
        functools.partial(total_kernel, n),
        out_shape=jax.ShapeDtypeStruct(part.shape, part.dtype),
        in_specs=[pl.BlockSpec(memory_space=pltpu.VMEM)],
        out_specs=pl.BlockSpec(memory_space=pltpu.VMEM),
        scratch_shapes=[pltpu.VMEM((n,) + part.shape, part.dtype), sems, sems],
        compiler_params=pltpu.CompilerParams(has_side_effects=True),
        cost_estimate=pl.CostEstimate(flops=0, bytes_accessed=8_000_000, transcendentals=0),
        name="change_sum",
    )(part)


def attend_kernel(first, keys, q_ref, rk_ref, rv_ref, k_ref, v_ref, out_ref):
    rows = q_ref.shape[0]
    nt = (((1,), (1,)), ((), ()))
    row = lax.broadcasted_iota(jnp.int32, (rows, keys), 0)
    col = lax.broadcasted_iota(jnp.int32, (rows, keys), 1)
    allowed = col <= row + first
    for half in range(2):
        cols = slice(half * HEAD_WIDTH, (half + 1) * HEAD_WIDTH)
        q = q_ref[:, cols]
        own = lax.dot_general(q, k_ref[:keys], nt, preferred_element_type=jnp.float32)
        own = jnp.where(allowed, jnp.exp(own), 0.0)
        read = jnp.exp(
            lax.dot_general(q, rk_ref[...], nt, preferred_element_type=jnp.float32)
        )
        denom = jnp.sum(own, axis=-1, keepdims=True) + jnp.sum(read, axis=-1, keepdims=True)
        numer = jnp.dot(
            own.astype(jnp.bfloat16), v_ref[:keys], preferred_element_type=jnp.float32
        ) + jnp.dot(read.astype(jnp.bfloat16), rv_ref[...], preferred_element_type=jnp.float32)
        out_ref[:, cols] = (numer / denom).astype(jnp.bfloat16)


def attend(q, read_k, read_v, local_k, local_v, first, keys):
    rows, width = q.shape
    mem, total = read_k.shape[0], local_k.shape[0]
    at = lambda h: (0, h)
    return pl.pallas_call(
        functools.partial(attend_kernel, first, keys),
        grid=(KEY_VALUE_HEADS,),
        out_shape=jax.ShapeDtypeStruct((rows, width), jnp.bfloat16),
        in_specs=[
            pl.BlockSpec((rows, 2 * HEAD_WIDTH), at),
            pl.BlockSpec((mem, HEAD_WIDTH), at),
            pl.BlockSpec((mem, HEAD_WIDTH), at),
            pl.BlockSpec((total, HEAD_WIDTH), at),
            pl.BlockSpec((total, HEAD_WIDTH), at),
        ],
        out_specs=pl.BlockSpec((rows, 2 * HEAD_WIDTH), at),
        cost_estimate=pl.CostEstimate(
            flops=4 * rows * width * (keys + mem), bytes_accessed=6_000_000, transcendentals=0
        ),
        name="attend",
    )(q, read_k, read_v, local_k, local_v)


def finish(inputs, attn, output_weight, post_gain):
    proj = jnp.dot(attn, output_weight, preferred_element_type=jnp.float32)
    mean_sq = jnp.mean(proj * proj, axis=-1, keepdims=True)
    return (inputs.astype(jnp.float32) + proj / jnp.sqrt(mean_sq + eps) * post_gain).astype(
        jnp.bfloat16
    )


def shards(
    tokens,
    memory,
    norm_gain,
    post_gain,
    query_weight,
    key_matrix,
    value_matrix,
    output_weight,
    segment_weight,
):
    n = lax.axis_size("seg")
    me = lax.axis_index("seg")
    tok_rows = tokens.shape[0]
    mem_rows, feature_width = memory.shape
    own_rows, query_width = query_weight.shape
    scale = 1.0 / HEAD_WIDTH**0.5
    output_full = lax.all_gather(output_weight, "seg", axis=0, tiled=True)

    mem_norm = prenorm(memory, norm_gain)
    own_cols = lax.dynamic_slice_in_dim(mem_norm, me * own_rows, own_rows, axis=1)
    part = jnp.dot(own_cols, query_weight, preferred_element_type=jnp.float32)
    blocks = query_width // LANES
    part = jnp.transpose(part.reshape(mem_rows, blocks, LANES), (1, 0, 2))
    core = lax.rem(me, 2)
    pairs = [(i, i + 1 - 2 * (i % 2)) for i in range(n)]
    share = blocks // 2
    kept = lax.dynamic_slice_in_dim(part, core * share, share, axis=0)
    given = lax.dynamic_slice_in_dim(part, (1 - core) * share, share, axis=0)
    kept = kept + lax.ppermute(given, "seg", pairs)
    peers = n // 2
    own_q = all_sum(kept.reshape(peers, mem_rows * share // peers, LANES), scale)
    own_q = own_q.reshape(share, mem_rows, LANES)
    other_q = lax.ppermute(own_q, "seg", pairs)
    low = core == 0
    write_q = jnp.concatenate(
        [jnp.where(low, own_q, other_q), jnp.where(low, other_q, own_q)], axis=0
    )
    write_q = jnp.transpose(write_q, (1, 0, 2)).reshape(mem_rows, query_width)

    own_query, write_q = lax.optimization_barrier((query_weight, write_q))
    query_full = lax.all_gather(own_query, "seg", axis=0, tiled=True)

    normed = prenorm(jnp.concatenate([tokens, memory], axis=0), norm_gain)
    local_k = jnp.dot(normed, key_matrix, preferred_element_type=jnp.float32).astype(jnp.bfloat16)
    local_v = jnp.dot(normed, value_matrix, preferred_element_type=jnp.float32).astype(jnp.bfloat16)
    total_rows = tok_rows + mem_rows
    first = jnp.int32(0) == me
    previous = memory
    squares = []
    own_weight = segment_weight[0]
    count_all = n * mem_rows * feature_width
    read_k, read_v = local_k[tok_rows:], local_v[tok_rows:]
    for step in range(ITERS):
        attn = attend(write_q, read_k, read_v, local_k, local_v, tok_rows, total_rows)
        newest = finish(memory, attn, output_full, post_gain)
        diff = newest.astype(jnp.float32) - previous.astype(jnp.float32)
        squares.append(jnp.sum(diff * diff) * own_weight)
        previous = newest
        if step + 1 < ITERS:
            read = jnp.where(first, memory, from_behind(newest, "seg", 1))
            read_norm = prenorm(read, norm_gain)
            read_k = jnp.dot(read_norm, key_matrix, preferred_element_type=jnp.float32).astype(
                jnp.bfloat16
            )
            read_v = jnp.dot(read_norm, value_matrix, preferred_element_type=jnp.float32).astype(
                jnp.bfloat16
            )
    squares = jnp.broadcast_to(jnp.pad(jnp.stack(squares), (0, LANES - ITERS))[None], (8, LANES))
    totals = small_sum(squares, n)[0, :ITERS]
    change_vec = jnp.sqrt(totals / count_all + eps)

    query_acc = jnp.dot(normed[:tok_rows], query_full, preferred_element_type=jnp.float32)
    query_vectors = (query_acc * scale).astype(jnp.bfloat16)
    attn = attend(query_vectors, read_k, read_v, local_k, local_v, 0, tok_rows)
    token_out = finish(tokens, attn, output_full, post_gain)
    return (token_out, previous, change_vec)


def chip_grid(chips):
    side = 1
    while (2 * side) ** 3 <= chips and chips % (4 * side * side) == 0:
        side *= 2
    return chips // (side * side), side


def fits(tokens, memory, norm_gain, post_gain, query_weight, *rest):
    n = lax.axis_size("seg")
    own_rows, query_width = query_weight.shape
    out_rows = rest[2].shape[0]
    mem_rows = memory.shape[0]
    if n % 2 or n < 8:
        return False
    _, side = chip_grid(n // 2)
    plane = 2 * side * side
    piece = mem_rows * (query_width // LANES) // n
    return (
        side == 2
        and own_rows % 16 == 0
        and out_rows % 16 == 0
        and (own_rows * plane) % LANES == 0
        and (out_rows * plane) % LANES == 0
        and own_rows > 16 * LAST_SLOW[1]
        and out_rows > 16 * LAST_SLOW[0]
        and piece % 16 == 0
        and mem_rows % piece == 0
        and memory.shape[1] >= 256
        and own_rows + LANES <= 256
    )


def nearest(position, k, size):
    value = 0
    for p in range(size):
        order = sorted(range(size), key=lambda q: (abs(q - p), q))
        value = jnp.where(position == p, order[k], value)
    return value


LAST_SLOW = (1, 1)
DUE = (
    (-11, 8, 13, 39, -2, 1),
    (-5, 14, 16, 22, 15, 1),
    (35, 13, 28, 71, -33, 1),
    (59, 16, 7, 14, 24, 0),
)
STEPS = (
    ("norm", -4),
    ("swap", -4),
    ("wk", 19),
    ("wv", 22),
    ("sum", 22),
    ("attend1", 60),
    ("p", (69, 69, 70, 70)),
    ("kv1", 70),
    ("a2", 85),
    ("kv2", 85),
    ("a3", 119),
    ("f3", 119),
    ("q", (136, 190, 222, 222)),
    ("tail", 222),
)


def make_plan(depth, side, groups):
    items = []
    for g in groups:
        base, by_k, by_j, by_i, both, lag = DUE[g]
        for k in range(depth):
            for j in range(side):
                for i in range(side):
                    due = base + by_k * k + by_j * j + by_i * i + both * j * i
                    items.append((due, -2, g, (k, j, i)))
                    if i == 0 and not (g % 2 and k):
                        items.append((due + lag, -1, g, (k, j, i)))
    last, count = -1000, 0
    for name, at in STEPS:
        for k in range(depth if isinstance(at, tuple) else 1):
            due = at[min(k, len(at) - 1)] if isinstance(at, tuple) else at
            last = max(last, due)
            items.append((last, count, name, k))
            count += 1
    items.sort(key=lambda t: (t[0], max(t[1], -1), t[1]))
    items = [(what, (which, order == -1)) if order < 0 else (what, which) for _, order, what, which in items]
    blocks = [t for t in items if isinstance(t[0], int)]
    plan = []

    def add(op):
        if op not in plan:
            plan.append(op)

    for what, which in items:
        if what in ("p", "q"):
            for g, e in blocks:
                if g // 2 == (what == "q") and e[0][0] == which:
                    add((g, e))
        add((what, which))
    return plan


def fused_kernel(
    n,
    tokens_hbm,
    memory_hbm,
    norm_gain,
    post_gain,
    wq_hbm,
    wk_hbm,
    wv_hbm,
    wo_hbm,
    seg_weight,
    token_out,
    memory_out,
    change_out,
    tokens,
    memory,
    wk,
    wv,
    wq,
    wo,
    window,
    normed,
    part,
    swapped,
    kept,
    held,
    piece_out,
    pieces,
    write_q,
    local_k,
    local_v,
    sent_kv,
    read_kv,
    attn,
    proj,
    previous,
    newnorm,
    query,
    change,
    changes,
    gains,
    load_sem,
    gather_send,
    gather_recv,
    pair_recv,
    swap_sem,
    sum_send,
    sum_recv,
    spread_send,
    spread_recv,
    kv_send,
    kv_recv,
    change_send,
    change_recv,
    store_sem,
):
    me = lax.axis_index("seg")
    barrier = pltpu.get_barrier_semaphore()

    @pl.loop(1, n)
    def _(k):
        to = lax.rem(me + k, n)
        pl.semaphore_signal(barrier, inc=1, device_id=(to,), device_id_type=MESH)

    core = lax.rem(me, 2)
    partner = me + 1 - 2 * core
    chip = me // 2
    chips = n // 2
    depth, side = chip_grid(chips)
    tok_rows, width = tokens.shape
    mem_rows = memory.shape[0]
    all_rows = tok_rows + mem_rows
    fast, mid, slow = (
        lax.rem(chip, side),
        lax.rem(chip // side, side),
        chip // (side * side),
    )
    scale = 1.0 / HEAD_WIDTH**0.5
    f32, bf16 = jnp.float32, jnp.bfloat16
    u = mid * (1 - core) + fast * core
    v = fast * (1 - core) + mid * core
    u_step = side * (1 - core) + core
    v_step = (1 - core) + side * core
    z_step = side * side
    full = (wo, wq)
    block_rows = (wo_hbm.shape[0], wq_hbm.shape[0])
    query_width = wq.shape[1]

    def hint(x, m):
        return pl.multiple_of(x, m)

    def block_at(w, device):
        rows = block_rows[w]
        return full[w].at[pl.ds(hint(device * rows, 16), rows)]

    cuts = [rows - 16 * LAST_SLOW[w] for w, rows in enumerate(block_rows)]
    groups = [g for g in range(4) if g % 2 == 0 or LAST_SLOW[g // 2]]

    def part_at(g, device):
        w, rest = g // 2, g % 2
        rows = 16 * LAST_SLOW[w] if rest else cuts[w]
        begin = device * block_rows[w] + (cuts[w] if rest else 0)
        return full[w].at[pl.ds(hint(begin, 16), rows)]

    def remote(src, dst, send, recv, device):
        return pltpu.make_async_remote_copy(
            src_ref=src,
            dst_ref=dst,
            send_sem=send,
            recv_sem=recv,
            device_id=(device,),
            device_id_type=MESH,
        )

    def place(k, j, i):
        z = nearest(slow, k, depth)
        uu = u if j == 0 else 1 - u
        vv = v if i == 0 else 1 - v
        return z, z * z_step + uu * u_step + vv * v_step

    def rank(k, j, i):
        return (k * side + j) * side + i

    def moves(g, k, j, i):
        z, origin = place(k, j, i)
        block = part_at(g, 2 * origin + core)
        last = g % 2
        ports = 5

        def copy(port, device, recv):
            return remote(
                block,
                block,
                gather_send.at[g, rank(k, j, i) * ports + port],
                recv.at[g, origin],
                device,
            )

        found = []
        if last or (j == 0 and i == 0):
            up = slow + 1 < depth
            down = slow > 0
            if k:
                up = jnp.logical_and(up, z < slow)
                down = jnp.logical_and(down, z > slow)
            found.append((up, copy(0, me + 2 * z_step, gather_recv)))
            found.append((down, copy(1, me - 2 * z_step, gather_recv)))
        if j == 0 and i == 0 and not (last and k):
            found.append((None, copy(2, me + 2 * u_step * (1 - 2 * u), gather_recv)))
        found.append((None, copy(4, partner, pair_recv)))
        if i == 0 and not (last and k):
            found.append((None, copy(3, me + 2 * v_step * (1 - 2 * v), gather_recv)))
        return found

    def start(items):
        for guard, copy in items:
            if guard is None:
                copy.start()
            else:
                pl.when(guard)(copy.start)

    def arrive(g, k, j, i):
        _, origin = place(k, j, i)
        block = part_at(g, 2 * origin + core)
        remote(
            block, block, gather_send.at[g, 0], gather_recv.at[g, origin], partner
        ).wait_recv()

    def take(g, e, onward):
        if onward:
            start(moves(g, *e)[-1:])
            return
        if any(e):
            arrive(g, *e)
        first = moves(g, *e)
        if e[2] == 0 and not (g % 2 and e[0]):
            first = first[:-1]
        start(first)

    def pair_arrive(w, slow_rank):
        for g in groups:
            if g // 2 == w:
                for j in range(side):
                    for i in range(side):
                        _, origin = place(slow_rank, j, i)
                        block = part_at(g, 2 * origin + 1 - core)
                        remote(
                            block,
                            block,
                            gather_send.at[g, 0],
                            pair_recv.at[g, origin],
                            partner,
                        ).wait_recv()

    def load(src, dst, i):
        return pltpu.make_async_copy(src, dst, load_sem.at[i])

    off = me * block_rows[1]
    first_lane = jnp.minimum(off // LANES * LANES, width - 256)
    shift = off - first_lane
    loads = [
        load(wo_hbm, block_at(0, me), 0),
        load(memory_hbm, memory, 1),
        load(wq_hbm, block_at(1, me), 2),
        load(tokens_hbm, tokens, 3),
        load(wk_hbm, wk, 4),
        load(wv_hbm, wv, 5),
    ]
    for copy in loads:
        copy.start()
    window[...] = jnp.zeros_like(window)
    own_window = load(
        wq_hbm, window.at[pl.ds(hint(shift, 16), block_rows[1])], 6
    )
    own_window.start()

    gains[0:1, :] = norm_gain[...].reshape(1, width)
    gains[1:2, :] = post_gain[...].reshape(1, width)

    def norm_rows(src, dst, at, rows):
        step_rows = 16

        @pl.loop(0, rows // step_rows)
        def _(t):
            here = pl.ds(hint(t * step_rows, step_rows), step_rows)
            x = src[here, :].astype(f32)
            mean_sq = jnp.sum(x * x, axis=-1, keepdims=True) / width
            there = pl.ds(hint(at + t * step_rows, step_rows), step_rows)
            dst[there, :] = (x / jnp.sqrt(mean_sq + eps) * gains[0:1, :]).astype(bf16)

    def times(lhs, weight, dst, tile):
        @pl.loop(0, weight.shape[1] // tile)
        def _(t):
            cols = pl.ds(hint(t * tile, tile), tile)
            dst[:, cols] = jnp.dot(
                lhs[...], weight[:, cols], preferred_element_type=f32
            ).astype(dst.dtype)

    nt = (((1,), (1,)), ((), ()))

    def attend_rows(q_ref, rows, rk, rv, first, keys, pre):
        row = lax.broadcasted_iota(jnp.int32, (rows, keys), 0)
        col = lax.broadcasted_iota(jnp.int32, (rows, keys), 1)
        allowed = col <= row + first

        @pl.loop(0, KEY_VALUE_HEADS)
        def _(g):
            kv_cols = pl.ds(hint(g * HEAD_WIDTH, HEAD_WIDTH), HEAD_WIDTH)
            kk = local_k[0:keys, kv_cols]
            vv = local_v[0:keys, kv_cols]
            rkk = rk[:, kv_cols]
            rvv = rv[:, kv_cols]
            for half in range(2):
                cols = pl.ds(hint((2 * g + half) * HEAD_WIDTH, HEAD_WIDTH), HEAD_WIDTH)
                q = q_ref[0:rows, cols]
                if pre:
                    q = (q * scale).astype(bf16)
                own = lax.dot_general(q, kk, nt, preferred_element_type=f32)
                own = jnp.where(allowed, jnp.exp(own), 0.0)
                read = jnp.exp(lax.dot_general(q, rkk, nt, preferred_element_type=f32))
                denom = jnp.sum(own, axis=-1, keepdims=True) + jnp.sum(
                    read, axis=-1, keepdims=True
                )
                numer = jnp.dot(
                    own.astype(bf16), vv, preferred_element_type=f32
                ) + jnp.dot(read.astype(bf16), rvv, preferred_element_type=f32)
                attn[0:rows, cols] = (numer / denom).astype(bf16)

    def project(rows):
        tile = 512

        @pl.loop(0, width // tile)
        def _(t):
            cols = pl.ds(hint(t * tile, tile), tile)
            proj[0:rows, cols] = jnp.dot(
                attn[0:rows, :], wo[:, cols], preferred_element_type=f32
            )

    out_rows = block_rows[0] * 2 * z_step

    def project_plane(k):
        at = hint(nearest(slow, k, depth) * out_rows, LANES)
        tile = 512

        @pl.loop(0, width // tile)
        def _(t):
            cols = pl.ds(hint(t * tile, tile), tile)
            more = jnp.dot(
                attn[0:mem_rows, pl.ds(at, out_rows)],
                wo[pl.ds(at, out_rows), cols],
                preferred_element_type=f32,
            )
            if k == 0:
                proj[0:mem_rows, cols] = more
            else:
                proj[0:mem_rows, cols] += more

    def layer_rows(src, here):
        p = proj[here, :]
        mean_sq = jnp.sum(p * p, axis=-1, keepdims=True) / width
        x = src[here, :].astype(f32)
        return (x + p / jnp.sqrt(mean_sq + eps) * gains[1:2, :]).astype(bf16)

    def write_rows(step):
        before = memory if step == 0 else previous
        change[...] = jnp.zeros_like(change) if step == 0 else change[...]
        lane = lax.broadcasted_iota(jnp.int32, change.shape, 1)

        @pl.loop(0, mem_rows // 16)
        def _(t):
            here = pl.ds(hint(t * 16, 16), 16)
            out = layer_rows(memory, here)
            o = out.astype(f32)
            diff = o - before[here, :].astype(f32)
            total = jnp.sum(diff * diff, keepdims=True)
            change[...] += jnp.where(lane == step, total * seg_weight[0], 0.0)
            previous[here, :] = out
            if step + 1 < ITERS:
                mean_sq = jnp.sum(o * o, axis=-1, keepdims=True) / width
                newnorm[here, :] = (o / jnp.sqrt(mean_sq + eps) * gains[0:1, :]).astype(bf16)

    right = lax.rem(me + 1, n)

    def kv_copy(step, which):
        return remote(
            sent_kv.at[step, which],
            read_kv.at[step, which],
            kv_send.at[step, which],
            kv_recv.at[step, which],
            right,
        )

    def send_kv(step):
        for which, weight in enumerate((wk, wv)):
            times(newnorm, weight, sent_kv.at[step, which], 512)
            pl.when(me + 1 < n)(kv_copy(step, which).start)

    def wait_kv(step):
        @pl.when(me > 0)
        def _():
            for which in range(2):
                kv_copy(step, which).wait_recv()

        @pl.when(me == 0)
        def _():
            for which, local in enumerate((local_k, local_v)):
                read_kv[step, which] = local[tok_rows:all_rows, :]

    piece = pieces.shape[1]
    per_block = mem_rows // piece
    half_width = query_width // 2
    swap = remote(part.at[1 - core], swapped, swap_sem.at[0], swap_sem.at[1], partner)

    def scatter(k):
        to = lax.rem(chip + k, chips)
        return remote(
            kept.at[to], held.at[k], sum_send.at[k], sum_recv.at[k], 2 * to + core
        )

    def spread(k):
        to = lax.rem(me + k, n)
        return remote(
            piece_out, pieces.at[me], spread_send.at[k], spread_recv.at[k], to
        )

    def share(k):
        to = lax.rem(me + k, n)
        return remote(change, changes.at[me], change_send.at[k], change_recv.at[k], to)

    def step_norm(_):
        loads[1].wait()
        norm_rows(memory, normed, tok_rows, mem_rows)
        own_window.wait()
        own_cols = normed[tok_rows:all_rows, pl.ds(hint(first_lane, LANES), 256)]
        for c in range(2):
            rows_of = jnp.dot(
                own_cols,
                window[:, c * half_width : (c + 1) * half_width],
                preferred_element_type=f32,
            )
            for t in range(chips):
                at = t // per_block * LANES
                down = t % per_block * piece
                part[c, t] = rows_of[down : down + piece, at : at + LANES]
        swap.start()

    def step_swap(_):
        loads[3].wait()
        norm_rows(tokens, normed, 0, tok_rows)
        swap.wait_recv()
        kept[...] = part[core] + swapped[...]

        @pl.loop(1, chips)
        def _(k):
            scatter(k).start()

    def step_wk(_):
        loads[4].wait()
        times(normed, wk, local_k, 512)

    def step_wv(_):
        loads[5].wait()
        times(normed, wv, local_v, 512)

    def step_sum(_):
        @pl.loop(1, chips)
        def _(k):
            scatter(k).wait_recv()

        piece_sum = kept[chip]
        for k in range(1, chips):
            piece_sum += held[k]
        piece_out[...] = (piece_sum * scale).astype(bf16)

        @pl.loop(1, n)
        def _(k):
            spread(k).start()

        pieces[me] = piece_out[...]

    def step_attend1(_):
        @pl.loop(1, n)
        def _(k):
            spread(k).wait_recv()

        for d in range(n):
            t, c = d // 2, d % 2
            at = c * half_width + t // per_block * LANES
            down = t % per_block * piece
            write_q[down : down + piece, at : at + LANES] = pieces[d]
        attend_rows(
            write_q,
            mem_rows,
            local_k.at[pl.ds(tok_rows, mem_rows)],
            local_v.at[pl.ds(tok_rows, mem_rows)],
            tok_rows,
            all_rows,
            False,
        )

    def step_p(k):
        pair_arrive(0, k)
        project_plane(k)

    def step_kv1(_):
        write_rows(0)
        send_kv(0)

    def attend_write(step):
        wait_kv(step)
        rk, rv = read_kv.at[step, 0], read_kv.at[step, 1]
        attend_rows(write_q, mem_rows, rk, rv, tok_rows, all_rows, False)

    def step_a2(_):
        attend_write(0)
        project(mem_rows)
        write_rows(1)

    def step_kv2(_):
        send_kv(1)

    def step_a3(_):
        attend_write(1)

    store = pltpu.make_async_copy(previous, memory_out, store_sem.at[0])

    def step_f3(_):
        project(mem_rows)
        write_rows(2)
        store.start()

        @pl.loop(1, n)
        def _(k):
            share(k).start()

        changes[me] = change[...]

    plane_rows = block_rows[1] * 2 * z_step

    def step_q(k):
        pair_arrive(1, k)
        at = hint(nearest(slow, k, depth) * plane_rows, LANES)
        tile = 512

        @pl.loop(0, query_width // tile)
        def _(t):
            cols = pl.ds(hint(t * tile, tile), tile)
            more = jnp.dot(
                normed[0:tok_rows, pl.ds(at, plane_rows)],
                wq[pl.ds(at, plane_rows), cols],
                preferred_element_type=f32,
            )
            if k == 0:
                query[:, cols] = more
            else:
                query[:, cols] += more

    store_tokens = pltpu.make_async_copy(tokens, token_out, store_sem.at[1])

    def step_tail(_):
        rk, rv = read_kv.at[ITERS - 2, 0], read_kv.at[ITERS - 2, 1]
        attend_rows(query, tok_rows, rk, rv, 0, tok_rows, True)
        project(tok_rows)

        @pl.loop(0, tok_rows // 16)
        def _(t):
            here = pl.ds(hint(t * 16, 16), 16)
            tokens[here, :] = layer_rows(tokens, here)

        store_tokens.start()

        @pl.loop(1, n)
        def _(k):
            share(k).wait_recv()

        count_all = n * mem_rows * width
        total = changes[0]
        for d in range(1, n):
            total += changes[d]
        change_out[...] = jnp.sqrt(total / count_all + eps)

    steps = {
        "norm": step_norm,
        "swap": step_swap,
        "wk": step_wk,
        "wv": step_wv,
        "sum": step_sum,
        "attend1": step_attend1,
        "p": step_p,
        "kv1": step_kv1,
        "a2": step_a2,
        "kv2": step_kv2,
        "a3": step_a3,
        "f3": step_f3,
        "q": step_q,
        "tail": step_tail,
    }
    plan = make_plan(depth, side, groups)
    loads[0].wait()
    pl.semaphore_wait(barrier, n - 1)
    fetched = False
    for what, which in plan:
        if what in steps:
            steps[what](which)
        else:
            if what // 2 and not fetched:
                loads[2].wait()
                fetched = True
            take(what, *which)

    swap.wait_send()
    for g, which in plan:
        if g in steps or which[1]:
            continue
        e = which[0]
        for guard, copy in moves(g, *e):
            if guard is None:
                copy.wait_send()
            else:
                pl.when(guard)(copy.wait_send)

    @pl.loop(1, chips)
    def _(k):
        scatter(k).wait_send()

    @pl.loop(1, n)
    def _(k):
        spread(k).wait_send()
        share(k).wait_send()

    @pl.when(me + 1 < n)
    def _():
        for step in range(ITERS - 1):
            for which in range(2):
                kv_copy(step, which).wait_send()

    store.wait()
    store_tokens.wait()


def fused(
    tokens,
    memory,
    norm_gain,
    post_gain,
    query_weight,
    key_matrix,
    value_matrix,
    output_weight,
    segment_weight,
):
    n = lax.axis_size("seg")
    chips = n // 2
    tok_rows, width = tokens.shape
    mem_rows = memory.shape[0]
    own_rows, query_width = query_weight.shape
    kv_width = key_matrix.shape[1]
    all_rows = tok_rows + mem_rows
    piece = mem_rows * (query_width // LANES) // n
    f32, bf16 = jnp.float32, jnp.bfloat16
    anywhere = pl.BlockSpec(memory_space=pl.ANY)
    in_vmem = pl.BlockSpec(memory_space=pltpu.VMEM)
    dma = pltpu.SemaphoreType.DMA
    outs = pl.pallas_call(
        functools.partial(fused_kernel, n),
        out_shape=(
            jax.ShapeDtypeStruct(tokens.shape, bf16),
            jax.ShapeDtypeStruct(memory.shape, bf16),
            jax.ShapeDtypeStruct((8, LANES), f32),
        ),
        in_specs=[
            anywhere,
            anywhere,
            in_vmem,
            in_vmem,
            anywhere,
            anywhere,
            anywhere,
            anywhere,
            pl.BlockSpec(memory_space=pltpu.SMEM),
        ],
        out_specs=(anywhere, anywhere, in_vmem),
        scratch_shapes=[
            pltpu.VMEM(tokens.shape, bf16),
            pltpu.VMEM(memory.shape, bf16),
            pltpu.VMEM(key_matrix.shape, bf16),
            pltpu.VMEM(value_matrix.shape, bf16),
            pltpu.VMEM((n * own_rows, query_width), bf16),
            pltpu.VMEM((query_width, width), bf16),
            pltpu.VMEM((256, query_width), bf16),
            pltpu.VMEM((all_rows, width), bf16),
            pltpu.VMEM((2, chips, piece, LANES), f32),
            pltpu.VMEM((chips, piece, LANES), f32),
            pltpu.VMEM((chips, piece, LANES), f32),
            pltpu.VMEM((chips, piece, LANES), f32),
            pltpu.VMEM((piece, LANES), bf16),
            pltpu.VMEM((n, piece, LANES), bf16),
            pltpu.VMEM((mem_rows, query_width), bf16),
            pltpu.VMEM((all_rows, kv_width), bf16),
            pltpu.VMEM((all_rows, kv_width), bf16),
            pltpu.VMEM((ITERS - 1, 2, mem_rows, kv_width), bf16),
            pltpu.VMEM((ITERS - 1, 2, mem_rows, kv_width), bf16),
            pltpu.VMEM((tok_rows, query_width), bf16),
            pltpu.VMEM((tok_rows, width), f32),
            pltpu.VMEM(memory.shape, bf16),
            pltpu.VMEM(memory.shape, bf16),
            pltpu.VMEM((tok_rows, query_width), f32),
            pltpu.VMEM((8, LANES), f32),
            pltpu.VMEM((n, 8, LANES), f32),
            pltpu.VMEM((2, width), f32),
            dma((7,)),
            dma((4, chips * 5)),
            dma((4, chips)),
            dma((4, chips)),
            dma((2,)),
            dma((chips,)),
            dma((chips,)),
            dma((n,)),
            dma((n,)),
            dma((ITERS - 1, 2)),
            dma((ITERS - 1, 2)),
            dma((n,)),
            dma((n,)),
            dma((2,)),
        ],
        compiler_params=pltpu.CompilerParams(
            collective_id=0, has_side_effects=True, vmem_limit_bytes=67_000_000
        ),
        name="segments",
    )(
        tokens,
        memory,
        norm_gain,
        post_gain,
        query_weight,
        key_matrix,
        value_matrix,
        output_weight,
        segment_weight,
    )
    return outs[0], outs[1], outs[2][0, :ITERS]


def solution(mesh):
    def step(*args):
        if fits(*args):
            return fused(*args)
        return shards(*args)

    in_specs = (
        P("seg", None),
        P(),
        P(),
        P(),
        P("seg", None),
        P(),
        P(),
        P("seg", None),
        P("seg"),
    )
    out_specs = (P("seg", None), P("seg", None), P())
    return jax.shard_map(
        step, mesh=mesh, in_specs=in_specs, out_specs=out_specs, check_vma=False
    )
```

```python
import functools

import jax
import jax.numpy as jnp
from jax import lax
from jax.experimental import pallas as pl
from jax.experimental.pallas import tpu as pltpu
from jax.sharding import PartitionSpec as P


HEAD_WIDTH = 256
KEY_VALUE_HEADS = 4
ITERS = 3
LANES = 128
MESH = pl.DeviceIdType.MESH


eps = 1e-06


def from_behind(block, axis, distance):
    devices = range(lax.axis_size(axis))
    route = [(i - distance, i) for i in devices if i - distance in devices]
    return lax.ppermute(block, axis, route)


def prenorm(rows, gain):
    rows = rows.astype(jnp.float32)
    mean_sq = jnp.mean(rows * rows, axis=-1, keepdims=True)
    return (rows / jnp.sqrt(mean_sq + eps) * gain).astype(jnp.bfloat16)


def reduce_kernel(n, scale, part_ref, out_ref, held, total, final, send1, recv1, send2, recv2):
    me = lax.axis_index("seg") // 2
    core = lax.rem(lax.axis_index("seg"), 2)

    def scatter(k):
        to = lax.rem(me + k, n)
        return pltpu.make_async_remote_copy(
            src_ref=part_ref.at[to],
            dst_ref=held.at[k],
            send_sem=send1.at[k],
            recv_sem=recv1.at[k],
            device_id=(2 * to + core,),
            device_id_type=MESH,
        )

    def spread(k):
        to = lax.rem(me + k, n)
        return pltpu.make_async_remote_copy(
            src_ref=final,
            dst_ref=out_ref.at[me],
            send_sem=send2.at[k],
            recv_sem=recv2.at[k],
            device_id=(2 * to + core,),
            device_id_type=MESH,
        )

    @pl.loop(1, n)
    def _(k):
        scatter(k).start()

    total[...] = part_ref[me]

    @pl.loop(1, n)
    def _(k):
        scatter(k).wait_recv()
        total[...] += held[k]

    final[...] = (total[...] * scale).astype(final.dtype)

    @pl.loop(1, n)
    def _(k):
        spread(k).start()

    out_ref[me] = final[...]

    @pl.loop(1, n)
    def _(k):
        scatter(k).wait_send()
        spread(k).wait()


def all_sum(parts, scale):
    n = parts.shape[0]
    sems = pltpu.SemaphoreType.DMA((n,))
    return pl.pallas_call(
        functools.partial(reduce_kernel, n, scale),
        out_shape=jax.ShapeDtypeStruct(parts.shape, jnp.bfloat16),
        in_specs=[pl.BlockSpec(memory_space=pltpu.VMEM)],
        out_specs=pl.BlockSpec(memory_space=pltpu.VMEM),
        scratch_shapes=[
            pltpu.VMEM(parts.shape, parts.dtype),
            pltpu.VMEM(parts.shape[1:], parts.dtype),
            pltpu.VMEM(parts.shape[1:], jnp.bfloat16),
            sems,
            sems,
            sems,
            sems,
        ],
        compiler_params=pltpu.CompilerParams(has_side_effects=True),
        cost_estimate=pl.CostEstimate(flops=0, bytes_accessed=30_000_000, transcendentals=0),
        name="query_sum",
    )(parts)


def total_kernel(n, part_ref, out_ref, held, send, recv):
    me = lax.axis_index("seg")

    def copy(k):
        return pltpu.make_async_remote_copy(
            src_ref=part_ref,
            dst_ref=held.at[me],
            send_sem=send.at[k],
            recv_sem=recv.at[k],
            device_id=(lax.rem(me + k, n),),
            device_id_type=MESH,
        )

    @pl.loop(1, n)
    def _(k):
        copy(k).start()

    held[me] = part_ref[...]

    @pl.loop(1, n)
    def _(k):
        copy(k).wait()

    out_ref[...] = jnp.sum(held[...], axis=0)


def small_sum(part, n):
    sems = pltpu.SemaphoreType.DMA((n,))
    return pl.pallas_call(
        functools.partial(total_kernel, n),
        out_shape=jax.ShapeDtypeStruct(part.shape, part.dtype),
        in_specs=[pl.BlockSpec(memory_space=pltpu.VMEM)],
        out_specs=pl.BlockSpec(memory_space=pltpu.VMEM),
        scratch_shapes=[pltpu.VMEM((n,) + part.shape, part.dtype), sems, sems],
        compiler_params=pltpu.CompilerParams(has_side_effects=True),
        cost_estimate=pl.CostEstimate(flops=0, bytes_accessed=8_000_000, transcendentals=0),
        name="change_sum",
    )(part)


def attend_kernel(first, keys, q_ref, rk_ref, rv_ref, k_ref, v_ref, out_ref):
    rows = q_ref.shape[0]
    nt = (((1,), (1,)), ((), ()))
    row = lax.broadcasted_iota(jnp.int32, (rows, keys), 0)
    col = lax.broadcasted_iota(jnp.int32, (rows, keys), 1)
    allowed = col <= row + first
    for half in range(2):
        cols = slice(half * HEAD_WIDTH, (half + 1) * HEAD_WIDTH)
        q = q_ref[:, cols]
        own = lax.dot_general(q, k_ref[:keys], nt, preferred_element_type=jnp.float32)
        own = jnp.where(allowed, jnp.exp(own), 0.0)
        read = jnp.exp(
            lax.dot_general(q, rk_ref[...], nt, preferred_element_type=jnp.float32)
        )
        denom = jnp.sum(own, axis=-1, keepdims=True) + jnp.sum(read, axis=-1, keepdims=True)
        numer = jnp.dot(
            own.astype(jnp.bfloat16), v_ref[:keys], preferred_element_type=jnp.float32
        ) + jnp.dot(read.astype(jnp.bfloat16), rv_ref[...], preferred_element_type=jnp.float32)
        out_ref[:, cols] = (numer / denom).astype(jnp.bfloat16)


def attend(q, read_k, read_v, local_k, local_v, first, keys):
    rows, width = q.shape
    mem, total = read_k.shape[0], local_k.shape[0]
    at = lambda h: (0, h)
    return pl.pallas_call(
        functools.partial(attend_kernel, first, keys),
        grid=(KEY_VALUE_HEADS,),
        out_shape=jax.ShapeDtypeStruct((rows, width), jnp.bfloat16),
        in_specs=[
            pl.BlockSpec((rows, 2 * HEAD_WIDTH), at),
            pl.BlockSpec((mem, HEAD_WIDTH), at),
            pl.BlockSpec((mem, HEAD_WIDTH), at),
            pl.BlockSpec((total, HEAD_WIDTH), at),
            pl.BlockSpec((total, HEAD_WIDTH), at),
        ],
        out_specs=pl.BlockSpec((rows, 2 * HEAD_WIDTH), at),
        cost_estimate=pl.CostEstimate(
            flops=4 * rows * width * (keys + mem), bytes_accessed=6_000_000, transcendentals=0
        ),
        name="attend",
    )(q, read_k, read_v, local_k, local_v)


def finish(inputs, attn, output_weight, post_gain):
    proj = jnp.dot(attn, output_weight, preferred_element_type=jnp.float32)
    mean_sq = jnp.mean(proj * proj, axis=-1, keepdims=True)
    return (inputs.astype(jnp.float32) + proj / jnp.sqrt(mean_sq + eps) * post_gain).astype(
        jnp.bfloat16
    )


def shards(
    tokens,
    memory,
    norm_gain,
    post_gain,
    query_weight,
    key_matrix,
    value_matrix,
    output_weight,
    segment_weight,
):
    n = lax.axis_size("seg")
    me = lax.axis_index("seg")
    tok_rows = tokens.shape[0]
    mem_rows, feature_width = memory.shape
    own_rows, query_width = query_weight.shape
    scale = 1.0 / HEAD_WIDTH**0.5
    output_full = lax.all_gather(output_weight, "seg", axis=0, tiled=True)

    mem_norm = prenorm(memory, norm_gain)
    own_cols = lax.dynamic_slice_in_dim(mem_norm, me * own_rows, own_rows, axis=1)
    part = jnp.dot(own_cols, query_weight, preferred_element_type=jnp.float32)
    blocks = query_width // LANES
    part = jnp.transpose(part.reshape(mem_rows, blocks, LANES), (1, 0, 2))
    core = lax.rem(me, 2)
    pairs = [(i, i + 1 - 2 * (i % 2)) for i in range(n)]
    share = blocks // 2
    kept = lax.dynamic_slice_in_dim(part, core * share, share, axis=0)
    given = lax.dynamic_slice_in_dim(part, (1 - core) * share, share, axis=0)
    kept = kept + lax.ppermute(given, "seg", pairs)
    peers = n // 2
    own_q = all_sum(kept.reshape(peers, mem_rows * share // peers, LANES), scale)
    own_q = own_q.reshape(share, mem_rows, LANES)
    other_q = lax.ppermute(own_q, "seg", pairs)
    low = core == 0
    write_q = jnp.concatenate(
        [jnp.where(low, own_q, other_q), jnp.where(low, other_q, own_q)], axis=0
    )
    write_q = jnp.transpose(write_q, (1, 0, 2)).reshape(mem_rows, query_width)

    own_query, write_q = lax.optimization_barrier((query_weight, write_q))
    query_full = lax.all_gather(own_query, "seg", axis=0, tiled=True)

    normed = prenorm(jnp.concatenate([tokens, memory], axis=0), norm_gain)
    local_k = jnp.dot(normed, key_matrix, preferred_element_type=jnp.float32).astype(jnp.bfloat16)
    local_v = jnp.dot(normed, value_matrix, preferred_element_type=jnp.float32).astype(jnp.bfloat16)
    total_rows = tok_rows + mem_rows
    first = jnp.int32(0) == me
    previous = memory
    squares = []
    own_weight = segment_weight[0]
    count_all = n * mem_rows * feature_width
    read_k, read_v = local_k[tok_rows:], local_v[tok_rows:]
    for step in range(ITERS):
        attn = attend(write_q, read_k, read_v, local_k, local_v, tok_rows, total_rows)
        newest = finish(memory, attn, output_full, post_gain)
        diff = newest.astype(jnp.float32) - previous.astype(jnp.float32)
        squares.append(jnp.sum(diff * diff) * own_weight)
        previous = newest
        if step + 1 < ITERS:
            read = jnp.where(first, memory, from_behind(newest, "seg", 1))
            read_norm = prenorm(read, norm_gain)
            read_k = jnp.dot(read_norm, key_matrix, preferred_element_type=jnp.float32).astype(
                jnp.bfloat16
            )
            read_v = jnp.dot(read_norm, value_matrix, preferred_element_type=jnp.float32).astype(
                jnp.bfloat16
            )
    squares = jnp.broadcast_to(jnp.pad(jnp.stack(squares), (0, LANES - ITERS))[None], (8, LANES))
    totals = small_sum(squares, n)[0, :ITERS]
    change_vec = jnp.sqrt(totals / count_all + eps)

    query_acc = jnp.dot(normed[:tok_rows], query_full, preferred_element_type=jnp.float32)
    query_vectors = (query_acc * scale).astype(jnp.bfloat16)
    attn = attend(query_vectors, read_k, read_v, local_k, local_v, 0, tok_rows)
    token_out = finish(tokens, attn, output_full, post_gain)
    return (token_out, previous, change_vec)


def chip_grid(chips):
    side = 1
    while (2 * side) ** 3 <= chips and chips % (4 * side * side) == 0:
        side *= 2
    return chips // (side * side), side


def fits(tokens, memory, norm_gain, post_gain, query_weight, *rest):
    n = lax.axis_size("seg")
    own_rows, query_width = query_weight.shape
    out_rows = rest[2].shape[0]
    mem_rows = memory.shape[0]
    if n % 2 or n < 8:
        return False
    _, side = chip_grid(n // 2)
    plane = 2 * side * side
    piece = mem_rows * (query_width // LANES) // n
    return (
        side == 2
        and own_rows % 16 == 0
        and out_rows % 16 == 0
        and (own_rows * plane) % LANES == 0
        and (out_rows * plane) % LANES == 0
        and own_rows > 16 * LAST_SLOW[1]
        and out_rows > 16 * LAST_SLOW[0]
        and piece % 16 == 0
        and tokens.shape[0] % 64 == 0
        and mem_rows % piece == 0
        and memory.shape[1] >= 256
        and own_rows + LANES <= 256
    )


def nearest(position, k, size):
    value = 0
    for p in range(size):
        order = sorted(range(size), key=lambda q: (abs(q - p), q))
        value = jnp.where(position == p, order[k], value)
    return value


TILE = 896
LAST_SLOW = (1, 1)
DUE = (
    (-11, 8, 13, 39, -2, 1),
    (-5, 14, 16, 22, 15, 1),
    (35, 13, 28, 71, -33, 1),
    (59, 16, 7, 14, 24, 0),
)
STEPS = (
    ("norm", -4),
    ("swap", -4),
    ("wk", 19),
    ("wv", 22),
    ("sum", 22),
    ("attend1", 60),
    ("p", (69, 69, 70, 70)),
    ("kv1", 70),
    ("a2", 85),
    ("kv2", 85),
    ("a3", 119),
    ("f3", 119),
    ("q", (136, 190, 222, 222)),
    ("tail", 222),
)


def make_plan(depth, side, groups):
    items = []
    for g in groups:
        base, by_k, by_j, by_i, both, lag = DUE[g]
        for k in range(depth):
            for j in range(side):
                for i in range(side):
                    due = base + by_k * k + by_j * j + by_i * i + both * j * i
                    items.append((due, -2, g, (k, j, i)))
                    if i == 0 and not (g % 2 and k):
                        items.append((due + lag, -1, g, (k, j, i)))
    last, count = -1000, 0
    for name, at in STEPS:
        for k in range(depth if isinstance(at, tuple) else 1):
            due = at[min(k, len(at) - 1)] if isinstance(at, tuple) else at
            last = max(last, due)
            items.append((last, count, name, k))
            count += 1
    items.sort(key=lambda t: (t[0], max(t[1], -1), t[1]))
    items = [(what, (which, order == -1)) if order < 0 else (what, which) for _, order, what, which in items]
    blocks = [t for t in items if isinstance(t[0], int)]
    plan = []

    def add(op):
        if op not in plan:
            plan.append(op)

    for what, which in items:
        if what in ("p", "q"):
            for g, e in blocks:
                if g // 2 == (what == "q") and e[0][0] == which:
                    add((g, e))
        add((what, which))
    return plan


def fused_kernel(
    n,
    tokens_hbm,
    memory_hbm,
    norm_gain,
    post_gain,
    wq_hbm,
    wk_hbm,
    wv_hbm,
    wo_hbm,
    seg_weight,
    token_out,
    memory_out,
    change_out,
    tokens,
    memory,
    wk,
    wv,
    wq,
    wo,
    window,
    normed,
    part,
    swapped,
    kept,
    held,
    piece_out,
    pieces,
    write_q,
    local_k,
    local_v,
    sent_kv,
    read_kv,
    attn,
    proj,
    previous,
    newnorm,
    query,
    change,
    changes,
    gains,
    squares,
    load_sem,
    gather_send,
    gather_recv,
    pair_recv,
    swap_sem,
    sum_send,
    sum_recv,
    spread_send,
    spread_recv,
    kv_send,
    kv_recv,
    change_send,
    change_recv,
    store_sem,
):
    me = lax.axis_index("seg")
    barrier = pltpu.get_barrier_semaphore()

    @pl.loop(1, n)
    def _(k):
        to = lax.rem(me + k, n)
        pl.semaphore_signal(barrier, inc=1, device_id=(to,), device_id_type=MESH)

    core = lax.rem(me, 2)
    partner = me + 1 - 2 * core
    chip = me // 2
    chips = n // 2
    depth, side = chip_grid(chips)
    tok_rows, width = tokens.shape
    mem_rows = memory.shape[0]
    all_rows = tok_rows + mem_rows
    fast, mid, slow = (
        lax.rem(chip, side),
        lax.rem(chip // side, side),
        chip // (side * side),
    )
    scale = 1.0 / HEAD_WIDTH**0.5
    f32, bf16 = jnp.float32, jnp.bfloat16
    u = mid * (1 - core) + fast * core
    v = fast * (1 - core) + mid * core
    u_step = side * (1 - core) + core
    v_step = (1 - core) + side * core
    z_step = side * side
    full = (wo, wq)
    block_rows = (wo_hbm.shape[0], wq_hbm.shape[0])
    query_width = wq.shape[1]

    def hint(x, m):
        return pl.multiple_of(x, m)

    def block_at(w, device):
        rows = block_rows[w]
        return full[w].at[pl.ds(hint(device * rows, 16), rows)]

    cuts = [rows - 16 * LAST_SLOW[w] for w, rows in enumerate(block_rows)]
    groups = [g for g in range(4) if g % 2 == 0 or LAST_SLOW[g // 2]]

    def part_at(g, device):
        w, rest = g // 2, g % 2
        rows = 16 * LAST_SLOW[w] if rest else cuts[w]
        begin = device * block_rows[w] + (cuts[w] if rest else 0)
        return full[w].at[pl.ds(hint(begin, 16), rows)]

    def remote(src, dst, send, recv, device):
        return pltpu.make_async_remote_copy(
            src_ref=src,
            dst_ref=dst,
            send_sem=send,
            recv_sem=recv,
            device_id=(device,),
            device_id_type=MESH,
        )

    def place(k, j, i):
        z = nearest(slow, k, depth)
        uu = u if j == 0 else 1 - u
        vv = v if i == 0 else 1 - v
        return z, z * z_step + uu * u_step + vv * v_step

    def rank(k, j, i):
        return (k * side + j) * side + i

    def moves(g, k, j, i):
        z, origin = place(k, j, i)
        block = part_at(g, 2 * origin + core)
        last = g % 2
        ports = 5

        def copy(port, device, recv):
            return remote(
                block,
                block,
                gather_send.at[g, rank(k, j, i) * ports + port],
                recv.at[g, origin],
                device,
            )

        found = []
        if last or (j == 0 and i == 0):
            up = slow + 1 < depth
            down = slow > 0
            if k:
                up = jnp.logical_and(up, z < slow)
                down = jnp.logical_and(down, z > slow)
            found.append((up, copy(0, me + 2 * z_step, gather_recv)))
            found.append((down, copy(1, me - 2 * z_step, gather_recv)))
        if j == 0 and i == 0 and not (last and k):
            found.append((None, copy(2, me + 2 * u_step * (1 - 2 * u), gather_recv)))
        found.append((None, copy(4, partner, pair_recv)))
        if i == 0 and not (last and k):
            found.append((None, copy(3, me + 2 * v_step * (1 - 2 * v), gather_recv)))
        return found

    def start(items):
        for guard, copy in items:
            if guard is None:
                copy.start()
            else:
                pl.when(guard)(copy.start)

    def arrive(g, k, j, i):
        _, origin = place(k, j, i)
        block = part_at(g, 2 * origin + core)
        remote(
            block, block, gather_send.at[g, 0], gather_recv.at[g, origin], partner
        ).wait_recv()

    def take(g, e, onward):
        if onward:
            start(moves(g, *e)[-1:])
            return
        if any(e):
            arrive(g, *e)
        first = moves(g, *e)
        if e[2] == 0 and not (g % 2 and e[0]):
            first = first[:-1]
        start(first)

    def pair_arrive(w, slow_rank):
        for g in groups:
            if g // 2 == w:
                for j in range(side):
                    for i in range(side):
                        _, origin = place(slow_rank, j, i)
                        block = part_at(g, 2 * origin + 1 - core)
                        remote(
                            block,
                            block,
                            gather_send.at[g, 0],
                            pair_recv.at[g, origin],
                            partner,
                        ).wait_recv()

    def load(src, dst, i):
        return pltpu.make_async_copy(src, dst, load_sem.at[i])

    off = me * block_rows[1]
    first_lane = jnp.minimum(off // LANES * LANES, width - 256)
    shift = off - first_lane
    loads = [
        load(wo_hbm, block_at(0, me), 0),
        load(memory_hbm, memory, 1),
        load(wq_hbm, block_at(1, me), 2),
        load(tokens_hbm, tokens, 3),
        load(wk_hbm, wk, 4),
        load(wv_hbm, wv, 5),
    ]
    for copy in loads:
        copy.start()
    window[...] = jnp.zeros_like(window)
    own_window = load(
        wq_hbm, window.at[pl.ds(hint(shift, 16), block_rows[1])], 6
    )
    own_window.start()

    gains[0:1, :] = norm_gain[...].reshape(1, width)
    gains[1:2, :] = post_gain[...].reshape(1, width)

    def norm_rows(src, dst, at, rows):
        step_rows = 16

        @pl.loop(0, rows // step_rows)
        def _(t):
            here = pl.ds(hint(t * step_rows, step_rows), step_rows)
            x = src[here, :].astype(f32)
            mean_sq = jnp.sum(x * x, axis=-1, keepdims=True) / width
            there = pl.ds(hint(at + t * step_rows, step_rows), step_rows)
            dst[there, :] = (x / jnp.sqrt(mean_sq + eps) * gains[0:1, :]).astype(bf16)

    def times(lhs, weight, dst, tile):
        @pl.loop(0, weight.shape[1] // tile)
        def _(t):
            cols = pl.ds(hint(t * tile, tile), tile)
            dst[:, cols] = jnp.dot(
                lhs[...], weight[:, cols], preferred_element_type=f32
            ).astype(dst.dtype)

    nt = (((1,), (1,)), ((), ()))

    def attend_rows(q_ref, rows, rk, rv, first, keys, pre):
        row = lax.broadcasted_iota(jnp.int32, (rows, keys), 0)
        col = lax.broadcasted_iota(jnp.int32, (rows, keys), 1)
        allowed = col <= row + first

        @pl.loop(0, KEY_VALUE_HEADS)
        def _(g):
            kv_cols = pl.ds(hint(g * HEAD_WIDTH, HEAD_WIDTH), HEAD_WIDTH)
            kk = local_k[0:keys, kv_cols]
            vv = local_v[0:keys, kv_cols]
            rkk = rk[:, kv_cols]
            rvv = rv[:, kv_cols]
            for half in range(2):
                cols = pl.ds(hint((2 * g + half) * HEAD_WIDTH, HEAD_WIDTH), HEAD_WIDTH)
                q = q_ref[0:rows, cols]
                if pre:
                    q = (q * scale).astype(bf16)
                own = lax.dot_general(q, kk, nt, preferred_element_type=f32)
                own = jnp.where(allowed, jnp.exp(own), 0.0)
                read = jnp.exp(lax.dot_general(q, rkk, nt, preferred_element_type=f32))
                denom = jnp.sum(own, axis=-1, keepdims=True) + jnp.sum(
                    read, axis=-1, keepdims=True
                )
                numer = jnp.dot(
                    own.astype(bf16), vv, preferred_element_type=f32
                ) + jnp.dot(read.astype(bf16), rvv, preferred_element_type=f32)
                attn[0:rows, cols] = (numer / denom).astype(bf16)

    def add_squares(rows, p, first):
        parts = p * p
        total = parts[:, 0:LANES]
        for c in range(LANES, p.shape[1], LANES):
            total += parts[:, c : c + LANES]

        @pl.when(first)
        def _():
            squares[0:rows, :] = total

        @pl.when(jnp.logical_not(first))
        def _():
            squares[0:rows, :] += total

    def project(rows):
        tile = TILE

        @pl.loop(0, width // tile)
        def _(t):
            cols = pl.ds(hint(t * tile, tile), tile)
            p = jnp.dot(attn[0:rows, :], wo[:, cols], preferred_element_type=f32)
            proj[0:rows, cols] = p
            add_squares(rows, p, t == 0)

    out_rows = block_rows[0] * 2 * z_step

    def project_plane(k):
        at = hint(nearest(slow, k, depth) * out_rows, LANES)
        tile = 512

        @pl.loop(0, width // tile)
        def _(t):
            cols = pl.ds(hint(t * tile, tile), tile)
            more = jnp.dot(
                attn[0:mem_rows, pl.ds(at, out_rows)],
                wo[pl.ds(at, out_rows), cols],
                preferred_element_type=f32,
            )
            if k == 0:
                proj[0:mem_rows, cols] = more
            else:
                more += proj[0:mem_rows, cols]
                proj[0:mem_rows, cols] = more
            if k == depth - 1:
                add_squares(mem_rows, more, t == 0)

    def divide_roots(rows):
        mean_sq = jnp.sum(squares[0:rows, :], axis=-1, keepdims=True) / width
        squares[0:rows, :] = jnp.broadcast_to(1.0 / jnp.sqrt(mean_sq + eps), (rows, LANES))

    def layer_rows(src, here):
        x = src[here, :].astype(f32)
        return (x + proj[here, :] * squares[here, 0:1] * gains[1:2, :]).astype(bf16)

    def write_rows(step):
        before = memory if step == 0 else previous
        change[...] = jnp.zeros_like(change) if step == 0 else change[...]
        lane = lax.broadcasted_iota(jnp.int32, change.shape, 1)
        divide_roots(mem_rows)

        @pl.loop(0, mem_rows // 16)
        def _(t):
            here = pl.ds(hint(t * 16, 16), 16)
            out = layer_rows(memory, here)
            o = out.astype(f32)
            diff = o - before[here, :].astype(f32)
            total = jnp.sum(diff * diff, keepdims=True)
            change[...] += jnp.where(lane == step, total * seg_weight[0], 0.0)
            previous[here, :] = out
            if step + 1 < ITERS:
                mean_sq = jnp.sum(o * o, axis=-1, keepdims=True) / width
                newnorm[here, :] = (o / jnp.sqrt(mean_sq + eps) * gains[0:1, :]).astype(bf16)

    right = lax.rem(me + 1, n)

    def kv_copy(step, which):
        return remote(
            sent_kv.at[step, which],
            read_kv.at[step, which],
            kv_send.at[step, which],
            kv_recv.at[step, which],
            right,
        )

    def send_kv(step):
        for which, weight in enumerate((wk, wv)):
            times(newnorm, weight, sent_kv.at[step, which], 512)
            pl.when(me + 1 < n)(kv_copy(step, which).start)

    def wait_kv(step):
        @pl.when(me > 0)
        def _():
            for which in range(2):
                kv_copy(step, which).wait_recv()

        @pl.when(me == 0)
        def _():
            for which, local in enumerate((local_k, local_v)):
                read_kv[step, which] = local[tok_rows:all_rows, :]

    piece = pieces.shape[2]
    per_block = mem_rows // piece
    half_width = query_width // 2
    swap = remote(part.at[1 - core], swapped, swap_sem.at[0], swap_sem.at[1], partner)

    def scatter(k):
        to = lax.rem(chip + k, chips)
        return remote(
            kept.at[to], held.at[k], sum_send.at[k], sum_recv.at[k], 2 * to + core
        )

    def spread(k):
        to = lax.rem(chip + k, chips)
        return remote(
            piece_out,
            pieces.at[core, chip],
            spread_send.at[k],
            spread_recv.at[k],
            2 * to + core,
        )

    hand_over = remote(
        pieces.at[core], pieces.at[core], swap_sem.at[2], swap_sem.at[3], partner
    )

    def share(k):
        to = lax.rem(me + k, n)
        return remote(change, changes.at[me], change_send.at[k], change_recv.at[k], to)

    def step_norm(_):
        loads[1].wait()
        norm_rows(memory, normed, tok_rows, mem_rows)
        own_window.wait()
        own_cols = normed[tok_rows:all_rows, pl.ds(hint(first_lane, LANES), 256)]
        for c in range(2):
            rows_of = jnp.dot(
                own_cols,
                window[:, c * half_width : (c + 1) * half_width],
                preferred_element_type=f32,
            )
            for t in range(chips):
                at = t // per_block * LANES
                down = t % per_block * piece
                part[c, t] = rows_of[down : down + piece, at : at + LANES]
        swap.start()

    def step_swap(_):
        loads[3].wait()
        norm_rows(tokens, normed, 0, tok_rows)
        swap.wait_recv()
        both = part[core] + swapped[...]
        kept[...] = both.astype(bf16)
        swapped[...] = both

        @pl.loop(1, chips)
        def _(k):
            scatter(k).start()

    def step_wk(_):
        loads[4].wait()
        times(normed, wk, local_k, 512)

    def step_wv(_):
        loads[5].wait()
        times(normed, wv, local_v, 512)

    def step_sum(_):
        @pl.loop(1, chips)
        def _(k):
            scatter(k).wait_recv()

        piece_sum = swapped[chip]
        for k in range(1, chips):
            piece_sum += held[k].astype(f32)
        piece_out[...] = (piece_sum * scale).astype(bf16)

        @pl.loop(1, chips)
        def _(k):
            spread(k).start()

        pieces[core, chip] = piece_out[...]

    def step_attend1(_):
        @pl.loop(1, chips)
        def _(k):
            spread(k).wait_recv()

        hand_over.start()
        hand_over.wait()
        for d in range(n):
            t, c = d // 2, d % 2
            at = c * half_width + t // per_block * LANES
            down = t % per_block * piece
            write_q[down : down + piece, at : at + LANES] = pieces[c, t]
        attend_rows(
            write_q,
            mem_rows,
            local_k.at[pl.ds(tok_rows, mem_rows)],
            local_v.at[pl.ds(tok_rows, mem_rows)],
            tok_rows,
            all_rows,
            False,
        )

    def step_p(k):
        pair_arrive(0, k)
        project_plane(k)

    def step_kv1(_):
        write_rows(0)
        send_kv(0)

    def attend_write(step):
        wait_kv(step)
        rk, rv = read_kv.at[step, 0], read_kv.at[step, 1]
        attend_rows(write_q, mem_rows, rk, rv, tok_rows, all_rows, False)

    def step_a2(_):
        attend_write(0)
        project(mem_rows)
        write_rows(1)

    def step_kv2(_):
        send_kv(1)

    def step_a3(_):
        attend_write(1)

    store = pltpu.make_async_copy(previous, memory_out, store_sem.at[0])

    def step_f3(_):
        project(mem_rows)
        write_rows(2)
        store.start()

        @pl.loop(1, n)
        def _(k):
            share(k).start()

        changes[me] = change[...]

    plane_rows = block_rows[1] * 2 * z_step

    def step_q(k):
        pair_arrive(1, k)
        at = hint(nearest(slow, k, depth) * plane_rows, LANES)
        tile = 512

        @pl.loop(0, query_width // tile)
        def _(t):
            cols = pl.ds(hint(t * tile, tile), tile)
            more = jnp.dot(
                normed[0:tok_rows, pl.ds(at, plane_rows)],
                wq[pl.ds(at, plane_rows), cols],
                preferred_element_type=f32,
            )
            if k == 0:
                query[:, cols] = more
            else:
                query[:, cols] += more

    chunk = tok_rows // 4

    def store_tokens(c):
        rows = pl.ds(c * chunk, chunk)
        return pltpu.make_async_copy(
            tokens.at[rows], token_out.at[rows], store_sem.at[1 + c]
        )

    def step_tail(_):
        rk, rv = read_kv.at[ITERS - 2, 0], read_kv.at[ITERS - 2, 1]
        attend_rows(query, tok_rows, rk, rv, 0, tok_rows, True)
        project(tok_rows)
        divide_roots(tok_rows)

        for c in range(4):

            @pl.loop(0, chunk // 16)
            def _(t):
                here = pl.ds(hint(c * chunk + t * 16, 16), 16)
                tokens[here, :] = layer_rows(tokens, here)

            store_tokens(c).start()

        @pl.loop(1, n)
        def _(k):
            share(k).wait_recv()

        count_all = n * mem_rows * width
        total = changes[0]
        for d in range(1, n):
            total += changes[d]
        change_out[...] = jnp.sqrt(total / count_all + eps)

    steps = {
        "norm": step_norm,
        "swap": step_swap,
        "wk": step_wk,
        "wv": step_wv,
        "sum": step_sum,
        "attend1": step_attend1,
        "p": step_p,
        "kv1": step_kv1,
        "a2": step_a2,
        "kv2": step_kv2,
        "a3": step_a3,
        "f3": step_f3,
        "q": step_q,
        "tail": step_tail,
    }
    plan = make_plan(depth, side, groups)
    loads[0].wait()
    pl.semaphore_wait(barrier, n - 1)
    fetched = False
    for what, which in plan:
        if what in steps:
            steps[what](which)
        else:
            if what // 2 and not fetched:
                loads[2].wait()
                fetched = True
            take(what, *which)

    swap.wait_send()
    for g, which in plan:
        if g in steps or which[1]:
            continue
        e = which[0]
        for guard, copy in moves(g, *e):
            if guard is None:
                copy.wait_send()
            else:
                pl.when(guard)(copy.wait_send)

    @pl.loop(1, chips)
    def _(k):
        scatter(k).wait_send()

        spread(k).wait_send()

    @pl.loop(1, n)
    def _(k):
        share(k).wait_send()

    @pl.when(me + 1 < n)
    def _():
        for step in range(ITERS - 1):
            for which in range(2):
                kv_copy(step, which).wait_send()

    store.wait()
    for c in range(4):
        store_tokens(c).wait()


def fused(
    tokens,
    memory,
    norm_gain,
    post_gain,
    query_weight,
    key_matrix,
    value_matrix,
    output_weight,
    segment_weight,
):
    n = lax.axis_size("seg")
    chips = n // 2
    tok_rows, width = tokens.shape
    mem_rows = memory.shape[0]
    own_rows, query_width = query_weight.shape
    kv_width = key_matrix.shape[1]
    all_rows = tok_rows + mem_rows
    piece = mem_rows * (query_width // LANES) // n
    f32, bf16 = jnp.float32, jnp.bfloat16
    anywhere = pl.BlockSpec(memory_space=pl.ANY)
    in_vmem = pl.BlockSpec(memory_space=pltpu.VMEM)
    dma = pltpu.SemaphoreType.DMA
    outs = pl.pallas_call(
        functools.partial(fused_kernel, n),
        out_shape=(
            jax.ShapeDtypeStruct(tokens.shape, bf16),
            jax.ShapeDtypeStruct(memory.shape, bf16),
            jax.ShapeDtypeStruct((8, LANES), f32),
        ),
        in_specs=[
            anywhere,
            anywhere,
            in_vmem,
            in_vmem,
            anywhere,
            anywhere,
            anywhere,
            anywhere,
            pl.BlockSpec(memory_space=pltpu.SMEM),
        ],
        out_specs=(anywhere, anywhere, in_vmem),
        scratch_shapes=[
            pltpu.VMEM(tokens.shape, bf16),
            pltpu.VMEM(memory.shape, bf16),
            pltpu.VMEM(key_matrix.shape, bf16),
            pltpu.VMEM(value_matrix.shape, bf16),
            pltpu.VMEM((n * own_rows, query_width), bf16),
            pltpu.VMEM((query_width, width), bf16),
            pltpu.VMEM((256, query_width), bf16),
            pltpu.VMEM((all_rows, width), bf16),
            pltpu.VMEM((2, chips, piece, LANES), f32),
            pltpu.VMEM((chips, piece, LANES), f32),
            pltpu.VMEM((chips, piece, LANES), bf16),
            pltpu.VMEM((chips, piece, LANES), bf16),
            pltpu.VMEM((piece, LANES), bf16),
            pltpu.VMEM((2, chips, piece, LANES), bf16),
            pltpu.VMEM((mem_rows, query_width), bf16),
            pltpu.VMEM((all_rows, kv_width), bf16),
            pltpu.VMEM((all_rows, kv_width), bf16),
            pltpu.VMEM((ITERS - 1, 2, mem_rows, kv_width), bf16),
            pltpu.VMEM((ITERS - 1, 2, mem_rows, kv_width), bf16),
            pltpu.VMEM((tok_rows, query_width), bf16),
            pltpu.VMEM((tok_rows, width), f32),
            pltpu.VMEM(memory.shape, bf16),
            pltpu.VMEM(memory.shape, bf16),
            pltpu.VMEM((tok_rows, query_width), f32),
            pltpu.VMEM((8, LANES), f32),
            pltpu.VMEM((n, 8, LANES), f32),
            pltpu.VMEM((2, width), f32),
            pltpu.VMEM((tok_rows, LANES), f32),
            dma((7,)),
            dma((4, chips * 5)),
            dma((4, chips)),
            dma((4, chips)),
            dma((4,)),
            dma((chips,)),
            dma((chips,)),
            dma((chips,)),
            dma((chips,)),
            dma((ITERS - 1, 2)),
            dma((ITERS - 1, 2)),
            dma((n,)),
            dma((n,)),
            dma((5,)),
        ],
        compiler_params=pltpu.CompilerParams(
            collective_id=0, has_side_effects=True, vmem_limit_bytes=67_000_000
        ),
        name="segments",
    )(
        tokens,
        memory,
        norm_gain,
        post_gain,
        query_weight,
        key_matrix,
        value_matrix,
        output_weight,
        segment_weight,
    )
    return outs[0], outs[1], outs[2][0, :ITERS]


def solution(mesh):
    def step(*args):
        if fits(*args):
            return fused(*args)
        return shards(*args)

    in_specs = (
        P("seg", None),
        P(),
        P(),
        P(),
        P("seg", None),
        P(),
        P(),
        P("seg", None),
        P("seg"),
    )
    out_specs = (P("seg", None), P("seg", None), P())
    return jax.shard_map(
        step, mesh=mesh, in_specs=in_specs, out_specs=out_specs, check_vma=False
    )
```

```python
import functools

import jax
import jax.numpy as jnp
from jax import lax
from jax.experimental import pallas as pl
from jax.experimental.pallas import tpu as pltpu
from jax.sharding import PartitionSpec as P


HEAD_WIDTH = 256
KEY_VALUE_HEADS = 4
ITERS = 3
LANES = 128
MESH = pl.DeviceIdType.MESH


eps = 1e-06


def from_behind(block, axis, distance):
    devices = range(lax.axis_size(axis))
    route = [(i - distance, i) for i in devices if i - distance in devices]
    return lax.ppermute(block, axis, route)


def prenorm(rows, gain):
    rows = rows.astype(jnp.float32)
    mean_sq = jnp.mean(rows * rows, axis=-1, keepdims=True)
    return (rows / jnp.sqrt(mean_sq + eps) * gain).astype(jnp.bfloat16)


def reduce_kernel(n, scale, part_ref, out_ref, held, total, final, send1, recv1, send2, recv2):
    me = lax.axis_index("seg") // 2
    core = lax.rem(lax.axis_index("seg"), 2)

    def scatter(k):
        to = lax.rem(me + k, n)
        return pltpu.make_async_remote_copy(
            src_ref=part_ref.at[to],
            dst_ref=held.at[k],
            send_sem=send1.at[k],
            recv_sem=recv1.at[k],
            device_id=(2 * to + core,),
            device_id_type=MESH,
        )

    def spread(k):
        to = lax.rem(me + k, n)
        return pltpu.make_async_remote_copy(
            src_ref=final,
            dst_ref=out_ref.at[me],
            send_sem=send2.at[k],
            recv_sem=recv2.at[k],
            device_id=(2 * to + core,),
            device_id_type=MESH,
        )

    @pl.loop(1, n)
    def _(k):
        scatter(k).start()

    total[...] = part_ref[me]

    @pl.loop(1, n)
    def _(k):
        scatter(k).wait_recv()
        total[...] += held[k]

    final[...] = (total[...] * scale).astype(final.dtype)

    @pl.loop(1, n)
    def _(k):
        spread(k).start()

    out_ref[me] = final[...]

    @pl.loop(1, n)
    def _(k):
        scatter(k).wait_send()
        spread(k).wait()


def all_sum(parts, scale):
    n = parts.shape[0]
    sems = pltpu.SemaphoreType.DMA((n,))
    return pl.pallas_call(
        functools.partial(reduce_kernel, n, scale),
        out_shape=jax.ShapeDtypeStruct(parts.shape, jnp.bfloat16),
        in_specs=[pl.BlockSpec(memory_space=pltpu.VMEM)],
        out_specs=pl.BlockSpec(memory_space=pltpu.VMEM),
        scratch_shapes=[
            pltpu.VMEM(parts.shape, parts.dtype),
            pltpu.VMEM(parts.shape[1:], parts.dtype),
            pltpu.VMEM(parts.shape[1:], jnp.bfloat16),
            sems,
            sems,
            sems,
            sems,
        ],
        compiler_params=pltpu.CompilerParams(has_side_effects=True),
        cost_estimate=pl.CostEstimate(flops=0, bytes_accessed=30_000_000, transcendentals=0),
        name="query_sum",
    )(parts)


def total_kernel(n, part_ref, out_ref, held, send, recv):
    me = lax.axis_index("seg")

    def copy(k):
        return pltpu.make_async_remote_copy(
            src_ref=part_ref,
            dst_ref=held.at[me],
            send_sem=send.at[k],
            recv_sem=recv.at[k],
            device_id=(lax.rem(me + k, n),),
            device_id_type=MESH,
        )

    @pl.loop(1, n)
    def _(k):
        copy(k).start()

    held[me] = part_ref[...]

    @pl.loop(1, n)
    def _(k):
        copy(k).wait()

    out_ref[...] = jnp.sum(held[...], axis=0)


def small_sum(part, n):
    sems = pltpu.SemaphoreType.DMA((n,))
    return pl.pallas_call(
        functools.partial(total_kernel, n),
        out_shape=jax.ShapeDtypeStruct(part.shape, part.dtype),
        in_specs=[pl.BlockSpec(memory_space=pltpu.VMEM)],
        out_specs=pl.BlockSpec(memory_space=pltpu.VMEM),
        scratch_shapes=[pltpu.VMEM((n,) + part.shape, part.dtype), sems, sems],
        compiler_params=pltpu.CompilerParams(has_side_effects=True),
        cost_estimate=pl.CostEstimate(flops=0, bytes_accessed=8_000_000, transcendentals=0),
        name="change_sum",
    )(part)


def attend_kernel(first, keys, q_ref, rk_ref, rv_ref, k_ref, v_ref, out_ref):
    rows = q_ref.shape[0]
    nt = (((1,), (1,)), ((), ()))
    row = lax.broadcasted_iota(jnp.int32, (rows, keys), 0)
    col = lax.broadcasted_iota(jnp.int32, (rows, keys), 1)
    allowed = col <= row + first
    for half in range(2):
        cols = slice(half * HEAD_WIDTH, (half + 1) * HEAD_WIDTH)
        q = q_ref[:, cols]
        own = lax.dot_general(q, k_ref[:keys], nt, preferred_element_type=jnp.float32)
        own = jnp.where(allowed, jnp.exp(own), 0.0)
        read = jnp.exp(
            lax.dot_general(q, rk_ref[...], nt, preferred_element_type=jnp.float32)
        )
        denom = jnp.sum(own, axis=-1, keepdims=True) + jnp.sum(read, axis=-1, keepdims=True)
        numer = jnp.dot(
            own.astype(jnp.bfloat16), v_ref[:keys], preferred_element_type=jnp.float32
        ) + jnp.dot(read.astype(jnp.bfloat16), rv_ref[...], preferred_element_type=jnp.float32)
        out_ref[:, cols] = (numer / denom).astype(jnp.bfloat16)


def attend(q, read_k, read_v, local_k, local_v, first, keys):
    rows, width = q.shape
    mem, total = read_k.shape[0], local_k.shape[0]
    at = lambda h: (0, h)
    return pl.pallas_call(
        functools.partial(attend_kernel, first, keys),
        grid=(KEY_VALUE_HEADS,),
        out_shape=jax.ShapeDtypeStruct((rows, width), jnp.bfloat16),
        in_specs=[
            pl.BlockSpec((rows, 2 * HEAD_WIDTH), at),
            pl.BlockSpec((mem, HEAD_WIDTH), at),
            pl.BlockSpec((mem, HEAD_WIDTH), at),
            pl.BlockSpec((total, HEAD_WIDTH), at),
            pl.BlockSpec((total, HEAD_WIDTH), at),
        ],
        out_specs=pl.BlockSpec((rows, 2 * HEAD_WIDTH), at),
        cost_estimate=pl.CostEstimate(
            flops=4 * rows * width * (keys + mem), bytes_accessed=6_000_000, transcendentals=0
        ),
        name="attend",
    )(q, read_k, read_v, local_k, local_v)


def finish(inputs, attn, output_weight, post_gain):
    proj = jnp.dot(attn, output_weight, preferred_element_type=jnp.float32)
    mean_sq = jnp.mean(proj * proj, axis=-1, keepdims=True)
    return (inputs.astype(jnp.float32) + proj / jnp.sqrt(mean_sq + eps) * post_gain).astype(
        jnp.bfloat16
    )


def shards(
    tokens,
    memory,
    norm_gain,
    post_gain,
    query_weight,
    key_matrix,
    value_matrix,
    output_weight,
    segment_weight,
):
    n = lax.axis_size("seg")
    me = lax.axis_index("seg")
    tok_rows = tokens.shape[0]
    mem_rows, feature_width = memory.shape
    own_rows, query_width = query_weight.shape
    scale = 1.0 / HEAD_WIDTH**0.5
    output_full = lax.all_gather(output_weight, "seg", axis=0, tiled=True)

    mem_norm = prenorm(memory, norm_gain)
    own_cols = lax.dynamic_slice_in_dim(mem_norm, me * own_rows, own_rows, axis=1)
    part = jnp.dot(own_cols, query_weight, preferred_element_type=jnp.float32)
    blocks = query_width // LANES
    part = jnp.transpose(part.reshape(mem_rows, blocks, LANES), (1, 0, 2))
    core = lax.rem(me, 2)
    pairs = [(i, i + 1 - 2 * (i % 2)) for i in range(n)]
    share = blocks // 2
    kept = lax.dynamic_slice_in_dim(part, core * share, share, axis=0)
    given = lax.dynamic_slice_in_dim(part, (1 - core) * share, share, axis=0)
    kept = kept + lax.ppermute(given, "seg", pairs)
    peers = n // 2
    own_q = all_sum(kept.reshape(peers, mem_rows * share // peers, LANES), scale)
    own_q = own_q.reshape(share, mem_rows, LANES)
    other_q = lax.ppermute(own_q, "seg", pairs)
    low = core == 0
    write_q = jnp.concatenate(
        [jnp.where(low, own_q, other_q), jnp.where(low, other_q, own_q)], axis=0
    )
    write_q = jnp.transpose(write_q, (1, 0, 2)).reshape(mem_rows, query_width)

    own_query, write_q = lax.optimization_barrier((query_weight, write_q))
    query_full = lax.all_gather(own_query, "seg", axis=0, tiled=True)

    normed = prenorm(jnp.concatenate([tokens, memory], axis=0), norm_gain)
    local_k = jnp.dot(normed, key_matrix, preferred_element_type=jnp.float32).astype(jnp.bfloat16)
    local_v = jnp.dot(normed, value_matrix, preferred_element_type=jnp.float32).astype(jnp.bfloat16)
    total_rows = tok_rows + mem_rows
    first = jnp.int32(0) == me
    previous = memory
    squares = []
    own_weight = segment_weight[0]
    count_all = n * mem_rows * feature_width
    read_k, read_v = local_k[tok_rows:], local_v[tok_rows:]
    for step in range(ITERS):
        attn = attend(write_q, read_k, read_v, local_k, local_v, tok_rows, total_rows)
        newest = finish(memory, attn, output_full, post_gain)
        diff = newest.astype(jnp.float32) - previous.astype(jnp.float32)
        squares.append(jnp.sum(diff * diff) * own_weight)
        previous = newest
        if step + 1 < ITERS:
            read = jnp.where(first, memory, from_behind(newest, "seg", 1))
            read_norm = prenorm(read, norm_gain)
            read_k = jnp.dot(read_norm, key_matrix, preferred_element_type=jnp.float32).astype(
                jnp.bfloat16
            )
            read_v = jnp.dot(read_norm, value_matrix, preferred_element_type=jnp.float32).astype(
                jnp.bfloat16
            )
    squares = jnp.broadcast_to(jnp.pad(jnp.stack(squares), (0, LANES - ITERS))[None], (8, LANES))
    totals = small_sum(squares, n)[0, :ITERS]
    change_vec = jnp.sqrt(totals / count_all + eps)

    query_acc = jnp.dot(normed[:tok_rows], query_full, preferred_element_type=jnp.float32)
    query_vectors = (query_acc * scale).astype(jnp.bfloat16)
    attn = attend(query_vectors, read_k, read_v, local_k, local_v, 0, tok_rows)
    token_out = finish(tokens, attn, output_full, post_gain)
    return (token_out, previous, change_vec)


def chip_grid(chips):
    side = 1
    while (2 * side) ** 3 <= chips and chips % (4 * side * side) == 0:
        side *= 2
    return chips // (side * side), side


def fits(tokens, memory, norm_gain, post_gain, query_weight, *rest):
    n = lax.axis_size("seg")
    own_rows, query_width = query_weight.shape
    out_rows = rest[2].shape[0]
    mem_rows = memory.shape[0]
    if n % 2 or n < 8:
        return False
    _, side = chip_grid(n // 2)
    plane = 2 * side * side
    piece = mem_rows * (query_width // LANES) // n
    return (
        side == 2
        and own_rows % 16 == 0
        and out_rows % 16 == 0
        and (own_rows * plane) % LANES == 0
        and (out_rows * plane) % LANES == 0
        and own_rows > 16 * LAST_SLOW[1]
        and out_rows > 16 * LAST_SLOW[0]
        and piece % 16 == 0
        and tokens.shape[0] % 64 == 0
        and mem_rows % piece == 0
        and memory.shape[1] >= 256
        and own_rows + LANES <= 256
    )


def nearest(position, k, size):
    value = 0
    for p in range(size):
        order = sorted(range(size), key=lambda q: (abs(q - p), q))
        value = jnp.where(position == p, order[k], value)
    return value


TILE = 896
LAST_SLOW = (1, 1)
DUE = (
    (-7, 9, 18, 77, 45, 1),
    (-5, 11, 20, 26, 80, 1),
    (24, 14, 38, 122, -24, 1),
    (32, 19, 24, 43, -27, 0),
)
STEPS = (
    ("norm", -2),
    ("swap", -2),
    ("wk", -2),
    ("wv", 18),
    ("sum", 18),
    ("attend1", 45),
    ("p", (45, 61, 64, 64)),
    ("kv1", 65),
    ("a2", 87),
    ("kv2", 89),
    ("a3", 143),
    ("f3", 169),
    ("q", (192, 254, 284, 284)),
    ("tail", 284),
)


def make_plan(depth, side, groups):
    items = []
    for g in groups:
        base, by_k, by_j, by_i, both, lag = DUE[g]
        for k in range(depth):
            for j in range(side):
                for i in range(side):
                    due = base + by_k * k + by_j * j + by_i * i + both * j * i
                    items.append((due, -2, g, (k, j, i)))
                    if i == 0 and not (g % 2 and k):
                        items.append((due + lag, -1, g, (k, j, i)))
    last, count = -1000, 0
    for name, at in STEPS:
        for k in range(depth if isinstance(at, tuple) else 1):
            due = at[min(k, len(at) - 1)] if isinstance(at, tuple) else at
            last = max(last, due)
            items.append((last, count, name, k))
            count += 1
    items.sort(key=lambda t: (t[0], max(t[1], -1), t[1]))
    items = [(what, (which, order == -1)) if order < 0 else (what, which) for _, order, what, which in items]
    blocks = [t for t in items if isinstance(t[0], int)]
    plan = []

    def add(op):
        if op not in plan:
            plan.append(op)

    for what, which in items:
        if what in ("p", "q"):
            for g, e in blocks:
                if g // 2 == (what == "q") and e[0][0] == which:
                    add((g, e))
        add((what, which))
    return plan


def fused_kernel(
    n,
    tokens_hbm,
    memory_hbm,
    norm_gain,
    post_gain,
    wq_hbm,
    wk_hbm,
    wv_hbm,
    wo_hbm,
    seg_weight,
    token_out,
    memory_out,
    change_out,
    tokens,
    memory,
    wk,
    wv,
    wq,
    wo,
    window,
    normed,
    part,
    swapped,
    kept,
    held,
    piece_out,
    pieces,
    write_q,
    local_k,
    local_v,
    sent_kv,
    read_kv,
    attn,
    proj,
    previous,
    newnorm,
    query,
    change,
    changes,
    gains,
    squares,
    load_sem,
    gather_send,
    gather_recv,
    pair_recv,
    swap_sem,
    sum_send,
    sum_recv,
    spread_send,
    spread_recv,
    kv_send,
    kv_recv,
    change_send,
    change_recv,
    store_sem,
):
    me = lax.axis_index("seg")
    barrier = pltpu.get_barrier_semaphore()

    @pl.loop(1, n)
    def _(k):
        to = lax.rem(me + k, n)
        pl.semaphore_signal(barrier, inc=1, device_id=(to,), device_id_type=MESH)

    core = lax.rem(me, 2)
    partner = me + 1 - 2 * core
    chip = me // 2
    chips = n // 2
    depth, side = chip_grid(chips)
    tok_rows, width = tokens.shape
    mem_rows = memory.shape[0]
    all_rows = tok_rows + mem_rows
    fast, mid, slow = (
        lax.rem(chip, side),
        lax.rem(chip // side, side),
        chip // (side * side),
    )
    scale = 1.0 / HEAD_WIDTH**0.5
    f32, bf16 = jnp.float32, jnp.bfloat16
    u = mid * (1 - core) + fast * core
    v = fast * (1 - core) + mid * core
    u_step = side * (1 - core) + core
    v_step = (1 - core) + side * core
    z_step = side * side
    full = (wo, wq)
    block_rows = (wo_hbm.shape[0], wq_hbm.shape[0])
    query_width = wq.shape[1]

    def hint(x, m):
        return pl.multiple_of(x, m)

    def block_at(w, device):
        rows = block_rows[w]
        return full[w].at[pl.ds(hint(device * rows, 16), rows)]

    cuts = [rows - 16 * LAST_SLOW[w] for w, rows in enumerate(block_rows)]
    groups = [g for g in range(4) if g % 2 == 0 or LAST_SLOW[g // 2]]

    def part_at(g, device):
        w, rest = g // 2, g % 2
        rows = 16 * LAST_SLOW[w] if rest else cuts[w]
        begin = device * block_rows[w] + (cuts[w] if rest else 0)
        return full[w].at[pl.ds(hint(begin, 16), rows)]

    def remote(src, dst, send, recv, device):
        return pltpu.make_async_remote_copy(
            src_ref=src,
            dst_ref=dst,
            send_sem=send,
            recv_sem=recv,
            device_id=(device,),
            device_id_type=MESH,
        )

    def place(k, j, i):
        z = nearest(slow, k, depth)
        uu = u if j == 0 else 1 - u
        vv = v if i == 0 else 1 - v
        return z, z * z_step + uu * u_step + vv * v_step

    def rank(k, j, i):
        return (k * side + j) * side + i

    def moves(g, k, j, i):
        z, origin = place(k, j, i)
        block = part_at(g, 2 * origin + core)
        last = g % 2
        ports = 5

        def copy(port, device, recv):
            return remote(
                block,
                block,
                gather_send.at[g, rank(k, j, i) * ports + port],
                recv.at[g, origin],
                device,
            )

        found = []
        if last or (j == 0 and i == 0):
            up = slow + 1 < depth
            down = slow > 0
            if k:
                up = jnp.logical_and(up, z < slow)
                down = jnp.logical_and(down, z > slow)
            found.append((up, copy(0, me + 2 * z_step, gather_recv)))
            found.append((down, copy(1, me - 2 * z_step, gather_recv)))
        if j == 0 and i == 0 and not (last and k):
            found.append((None, copy(2, me + 2 * u_step * (1 - 2 * u), gather_recv)))
        found.append((None, copy(4, partner, pair_recv)))
        if i == 0 and not (last and k):
            found.append((None, copy(3, me + 2 * v_step * (1 - 2 * v), gather_recv)))
        return found

    def start(items):
        for guard, copy in items:
            if guard is None:
                copy.start()
            else:
                pl.when(guard)(copy.start)

    def arrive(g, k, j, i):
        _, origin = place(k, j, i)
        block = part_at(g, 2 * origin + core)
        remote(
            block, block, gather_send.at[g, 0], gather_recv.at[g, origin], partner
        ).wait_recv()

    def take(g, e, onward):
        if onward:
            start(moves(g, *e)[-1:])
            return
        if any(e):
            arrive(g, *e)
        first = moves(g, *e)
        if e[2] == 0 and not (g % 2 and e[0]):
            first = first[:-1]
        start(first)

    def pair_arrive(w, slow_rank):
        for g in groups:
            if g // 2 == w:
                for j in range(side):
                    for i in range(side):
                        _, origin = place(slow_rank, j, i)
                        block = part_at(g, 2 * origin + 1 - core)
                        remote(
                            block,
                            block,
                            gather_send.at[g, 0],
                            pair_recv.at[g, origin],
                            partner,
                        ).wait_recv()

    def load(src, dst, i):
        return pltpu.make_async_copy(src, dst, load_sem.at[i])

    off = me * block_rows[1]
    first_lane = jnp.minimum(off // LANES * LANES, width - 256)
    shift = off - first_lane
    loads = [
        load(wo_hbm, block_at(0, me), 0),
        load(memory_hbm, memory, 1),
        load(wq_hbm, block_at(1, me), 2),
        load(tokens_hbm, tokens, 3),
        load(wk_hbm, wk, 4),
        load(wv_hbm, wv, 5),
    ]
    for copy in loads:
        copy.start()
    window[...] = jnp.zeros_like(window)
    own_window = load(
        wq_hbm, window.at[pl.ds(hint(shift, 16), block_rows[1])], 6
    )
    own_window.start()

    gains[0:1, :] = norm_gain[...].reshape(1, width)
    gains[1:2, :] = post_gain[...].reshape(1, width)

    def norm_rows(src, dst, at, rows):
        step_rows = 16

        @pl.loop(0, rows // step_rows)
        def _(t):
            here = pl.ds(hint(t * step_rows, step_rows), step_rows)
            x = src[here, :].astype(f32)
            mean_sq = jnp.sum(x * x, axis=-1, keepdims=True) / width
            there = pl.ds(hint(at + t * step_rows, step_rows), step_rows)
            dst[there, :] = (x / jnp.sqrt(mean_sq + eps) * gains[0:1, :]).astype(bf16)

    def times(lhs, weight, dst, tile):
        @pl.loop(0, weight.shape[1] // tile)
        def _(t):
            cols = pl.ds(hint(t * tile, tile), tile)
            dst[:, cols] = jnp.dot(
                lhs[...], weight[:, cols], preferred_element_type=f32
            ).astype(dst.dtype)

    nt = (((1,), (1,)), ((), ()))

    def attend_rows(q_ref, rows, rk, rv, first, keys, pre):
        row = lax.broadcasted_iota(jnp.int32, (rows, keys), 0)
        col = lax.broadcasted_iota(jnp.int32, (rows, keys), 1)
        allowed = col <= row + first

        @pl.loop(0, KEY_VALUE_HEADS)
        def _(g):
            kv_cols = pl.ds(hint(g * HEAD_WIDTH, HEAD_WIDTH), HEAD_WIDTH)
            kk = local_k[0:keys, kv_cols]
            vv = local_v[0:keys, kv_cols]
            rkk = rk[:, kv_cols]
            rvv = rv[:, kv_cols]
            for half in range(2):
                cols = pl.ds(hint((2 * g + half) * HEAD_WIDTH, HEAD_WIDTH), HEAD_WIDTH)
                q = q_ref[0:rows, cols]
                if pre:
                    q = (q * scale).astype(bf16)
                own = lax.dot_general(q, kk, nt, preferred_element_type=f32)
                own = jnp.where(allowed, jnp.exp(own), 0.0)
                read = jnp.exp(lax.dot_general(q, rkk, nt, preferred_element_type=f32))
                denom = jnp.sum(own, axis=-1, keepdims=True) + jnp.sum(
                    read, axis=-1, keepdims=True
                )
                numer = jnp.dot(
                    own.astype(bf16), vv, preferred_element_type=f32
                ) + jnp.dot(read.astype(bf16), rvv, preferred_element_type=f32)
                attn[0:rows, cols] = (numer / denom).astype(bf16)

    def add_squares(rows, p, first):
        parts = p * p
        total = parts[:, 0:LANES]
        for c in range(LANES, p.shape[1], LANES):
            total += parts[:, c : c + LANES]

        @pl.when(first)
        def _():
            squares[0:rows, :] = total

        @pl.when(jnp.logical_not(first))
        def _():
            squares[0:rows, :] += total

    def project(rows):
        tile = TILE

        @pl.loop(0, width // tile)
        def _(t):
            cols = pl.ds(hint(t * tile, tile), tile)
            p = jnp.dot(attn[0:rows, :], wo[:, cols], preferred_element_type=f32)
            proj[0:rows, cols] = p
            add_squares(rows, p, t == 0)

    out_rows = block_rows[0] * 2 * z_step

    def project_plane(k):
        at = hint(nearest(slow, k, depth) * out_rows, LANES)
        tile = 512

        @pl.loop(0, width // tile)
        def _(t):
            cols = pl.ds(hint(t * tile, tile), tile)
            more = jnp.dot(
                attn[0:mem_rows, pl.ds(at, out_rows)],
                wo[pl.ds(at, out_rows), cols],
                preferred_element_type=f32,
            )
            if k == 0:
                proj[0:mem_rows, cols] = more
            else:
                more += proj[0:mem_rows, cols]
                proj[0:mem_rows, cols] = more
            if k == depth - 1:
                add_squares(mem_rows, more, t == 0)

    def divide_roots(rows):
        mean_sq = jnp.sum(squares[0:rows, :], axis=-1, keepdims=True) / width
        squares[0:rows, :] = jnp.broadcast_to(1.0 / jnp.sqrt(mean_sq + eps), (rows, LANES))

    def layer_rows(src, here):
        x = src[here, :].astype(f32)
        return (x + proj[here, :] * squares[here, 0:1] * gains[1:2, :]).astype(bf16)

    def write_rows(step):
        before = memory if step == 0 else previous
        change[...] = jnp.zeros_like(change) if step == 0 else change[...]
        lane = lax.broadcasted_iota(jnp.int32, change.shape, 1)
        divide_roots(mem_rows)

        @pl.loop(0, mem_rows // 16)
        def _(t):
            here = pl.ds(hint(t * 16, 16), 16)
            out = layer_rows(memory, here)
            o = out.astype(f32)
            diff = o - before[here, :].astype(f32)
            total = jnp.sum(diff * diff, keepdims=True)
            change[...] += jnp.where(lane == step, total * seg_weight[0], 0.0)
            previous[here, :] = out
            if step + 1 < ITERS:
                mean_sq = jnp.sum(o * o, axis=-1, keepdims=True) / width
                newnorm[here, :] = (o / jnp.sqrt(mean_sq + eps) * gains[0:1, :]).astype(bf16)

    right = lax.rem(me + 1, n)

    def kv_copy(step, which):
        return remote(
            sent_kv.at[step, which],
            read_kv.at[step, which],
            kv_send.at[step, which],
            kv_recv.at[step, which],
            right,
        )

    def send_kv(step):
        for which, weight in enumerate((wk, wv)):
            times(newnorm, weight, sent_kv.at[step, which], 512)
            pl.when(me + 1 < n)(kv_copy(step, which).start)

    def wait_kv(step):
        @pl.when(me > 0)
        def _():
            for which in range(2):
                kv_copy(step, which).wait_recv()

        @pl.when(me == 0)
        def _():
            for which, local in enumerate((local_k, local_v)):
                read_kv[step, which] = local[tok_rows:all_rows, :]

    piece = pieces.shape[2]
    per_block = mem_rows // piece
    half_width = query_width // 2
    swap = remote(part.at[1 - core], swapped, swap_sem.at[0], swap_sem.at[1], partner)

    def scatter(k):
        to = lax.rem(chip + k, chips)
        return remote(
            kept.at[to], held.at[k], sum_send.at[k], sum_recv.at[k], 2 * to + core
        )

    def spread(k):
        to = lax.rem(chip + k, chips)
        return remote(
            piece_out,
            pieces.at[core, chip],
            spread_send.at[k],
            spread_recv.at[k],
            2 * to + core,
        )

    hand_over = remote(
        pieces.at[core], pieces.at[core], swap_sem.at[2], swap_sem.at[3], partner
    )

    def share(k):
        to = lax.rem(me + k, n)
        return remote(change, changes.at[me], change_send.at[k], change_recv.at[k], to)

    def step_norm(_):
        loads[1].wait()
        norm_rows(memory, normed, tok_rows, mem_rows)
        own_window.wait()
        own_cols = normed[tok_rows:all_rows, pl.ds(hint(first_lane, LANES), 256)]
        for c in range(2):
            rows_of = jnp.dot(
                own_cols,
                window[:, c * half_width : (c + 1) * half_width],
                preferred_element_type=f32,
            )
            for t in range(chips):
                at = t // per_block * LANES
                down = t % per_block * piece
                part[c, t] = rows_of[down : down + piece, at : at + LANES]
        swap.start()

    def step_swap(_):
        loads[3].wait()
        norm_rows(tokens, normed, 0, tok_rows)
        swap.wait_recv()
        both = part[core] + swapped[...]
        kept[...] = both.astype(bf16)
        swapped[...] = both

        @pl.loop(1, chips)
        def _(k):
            scatter(k).start()

    def step_wk(_):
        loads[4].wait()
        times(normed, wk, local_k, 512)

    def step_wv(_):
        loads[5].wait()
        times(normed, wv, local_v, 512)

    def step_sum(_):
        @pl.loop(1, chips)
        def _(k):
            scatter(k).wait_recv()

        piece_sum = swapped[chip]
        for k in range(1, chips):
            piece_sum += held[k].astype(f32)
        piece_out[...] = (piece_sum * scale).astype(bf16)

        @pl.loop(1, chips)
        def _(k):
            spread(k).start()

        pieces[core, chip] = piece_out[...]

    def step_attend1(_):
        @pl.loop(1, chips)
        def _(k):
            spread(k).wait_recv()

        hand_over.start()
        hand_over.wait()
        for d in range(n):
            t, c = d // 2, d % 2
            at = c * half_width + t // per_block * LANES
            down = t % per_block * piece
            write_q[down : down + piece, at : at + LANES] = pieces[c, t]
        attend_rows(
            write_q,
            mem_rows,
            local_k.at[pl.ds(tok_rows, mem_rows)],
            local_v.at[pl.ds(tok_rows, mem_rows)],
            tok_rows,
            all_rows,
            False,
        )

    def step_p(k):
        pair_arrive(0, k)
        project_plane(k)

    def step_kv1(_):
        write_rows(0)
        send_kv(0)

    def attend_write(step):
        wait_kv(step)
        rk, rv = read_kv.at[step, 0], read_kv.at[step, 1]
        attend_rows(write_q, mem_rows, rk, rv, tok_rows, all_rows, False)

    def step_a2(_):
        attend_write(0)
        project(mem_rows)
        write_rows(1)

    def step_kv2(_):
        send_kv(1)

    def step_a3(_):
        attend_write(1)

    store = pltpu.make_async_copy(previous, memory_out, store_sem.at[0])

    def step_f3(_):
        project(mem_rows)
        write_rows(2)
        store.start()

        @pl.loop(1, n)
        def _(k):
            share(k).start()

        changes[me] = change[...]

    plane_rows = block_rows[1] * 2 * z_step

    def step_q(k):
        pair_arrive(1, k)
        at = hint(nearest(slow, k, depth) * plane_rows, LANES)
        tile = 512

        @pl.loop(0, query_width // tile)
        def _(t):
            cols = pl.ds(hint(t * tile, tile), tile)
            more = jnp.dot(
                normed[0:tok_rows, pl.ds(at, plane_rows)],
                wq[pl.ds(at, plane_rows), cols],
                preferred_element_type=f32,
            )
            if k == 0:
                query[:, cols] = more
            else:
                query[:, cols] += more

    chunk = tok_rows // 4

    def store_tokens(c):
        rows = pl.ds(c * chunk, chunk)
        return pltpu.make_async_copy(
            tokens.at[rows], token_out.at[rows], store_sem.at[1 + c]
        )

    def step_tail(_):
        rk, rv = read_kv.at[ITERS - 2, 0], read_kv.at[ITERS - 2, 1]
        attend_rows(query, tok_rows, rk, rv, 0, tok_rows, True)
        project(tok_rows)
        divide_roots(tok_rows)

        for c in range(4):

            @pl.loop(0, chunk // 16)
            def _(t):
                here = pl.ds(hint(c * chunk + t * 16, 16), 16)
                tokens[here, :] = layer_rows(tokens, here)

            store_tokens(c).start()

        @pl.loop(1, n)
        def _(k):
            share(k).wait_recv()

        count_all = n * mem_rows * width
        total = changes[0]
        for d in range(1, n):
            total += changes[d]
        change_out[...] = jnp.sqrt(total / count_all + eps)

    steps = {
        "norm": step_norm,
        "swap": step_swap,
        "wk": step_wk,
        "wv": step_wv,
        "sum": step_sum,
        "attend1": step_attend1,
        "p": step_p,
        "kv1": step_kv1,
        "a2": step_a2,
        "kv2": step_kv2,
        "a3": step_a3,
        "f3": step_f3,
        "q": step_q,
        "tail": step_tail,
    }
    plan = make_plan(depth, side, groups)
    loads[0].wait()
    pl.semaphore_wait(barrier, n - 1)
    fetched = False
    for what, which in plan:
        if what in steps:
            steps[what](which)
        else:
            if what // 2 and not fetched:
                loads[2].wait()
                fetched = True
            take(what, *which)

    swap.wait_send()
    for g, which in plan:
        if g in steps or which[1]:
            continue
        e = which[0]
        for guard, copy in moves(g, *e):
            if guard is None:
                copy.wait_send()
            else:
                pl.when(guard)(copy.wait_send)

    @pl.loop(1, chips)
    def _(k):
        scatter(k).wait_send()

        spread(k).wait_send()

    @pl.loop(1, n)
    def _(k):
        share(k).wait_send()

    @pl.when(me + 1 < n)
    def _():
        for step in range(ITERS - 1):
            for which in range(2):
                kv_copy(step, which).wait_send()

    store.wait()
    for c in range(4):
        store_tokens(c).wait()


def fused(
    tokens,
    memory,
    norm_gain,
    post_gain,
    query_weight,
    key_matrix,
    value_matrix,
    output_weight,
    segment_weight,
):
    n = lax.axis_size("seg")
    chips = n // 2
    tok_rows, width = tokens.shape
    mem_rows = memory.shape[0]
    own_rows, query_width = query_weight.shape
    kv_width = key_matrix.shape[1]
    all_rows = tok_rows + mem_rows
    piece = mem_rows * (query_width // LANES) // n
    f32, bf16 = jnp.float32, jnp.bfloat16
    anywhere = pl.BlockSpec(memory_space=pl.ANY)
    in_vmem = pl.BlockSpec(memory_space=pltpu.VMEM)
    dma = pltpu.SemaphoreType.DMA
    outs = pl.pallas_call(
        functools.partial(fused_kernel, n),
        out_shape=(
            jax.ShapeDtypeStruct(tokens.shape, bf16),
            jax.ShapeDtypeStruct(memory.shape, bf16),
            jax.ShapeDtypeStruct((8, LANES), f32),
        ),
        in_specs=[
            anywhere,
            anywhere,
            in_vmem,
            in_vmem,
            anywhere,
            anywhere,
            anywhere,
            anywhere,
            pl.BlockSpec(memory_space=pltpu.SMEM),
        ],
        out_specs=(anywhere, anywhere, in_vmem),
        scratch_shapes=[
            pltpu.VMEM(tokens.shape, bf16),
            pltpu.VMEM(memory.shape, bf16),
            pltpu.VMEM(key_matrix.shape, bf16),
            pltpu.VMEM(value_matrix.shape, bf16),
            pltpu.VMEM((n * own_rows, query_width), bf16),
            pltpu.VMEM((query_width, width), bf16),
            pltpu.VMEM((256, query_width), bf16),
            pltpu.VMEM((all_rows, width), bf16),
            pltpu.VMEM((2, chips, piece, LANES), f32),
            pltpu.VMEM((chips, piece, LANES), f32),
            pltpu.VMEM((chips, piece, LANES), bf16),
            pltpu.VMEM((chips, piece, LANES), bf16),
            pltpu.VMEM((piece, LANES), bf16),
            pltpu.VMEM((2, chips, piece, LANES), bf16),
            pltpu.VMEM((mem_rows, query_width), bf16),
            pltpu.VMEM((all_rows, kv_width), bf16),
            pltpu.VMEM((all_rows, kv_width), bf16),
            pltpu.VMEM((ITERS - 1, 2, mem_rows, kv_width), bf16),
            pltpu.VMEM((ITERS - 1, 2, mem_rows, kv_width), bf16),
            pltpu.VMEM((tok_rows, query_width), bf16),
            pltpu.VMEM((tok_rows, width), f32),
            pltpu.VMEM(memory.shape, bf16),
            pltpu.VMEM(memory.shape, bf16),
            pltpu.VMEM((tok_rows, query_width), f32),
            pltpu.VMEM((8, LANES), f32),
            pltpu.VMEM((n, 8, LANES), f32),
            pltpu.VMEM((2, width), f32),
            pltpu.VMEM((tok_rows, LANES), f32),
            dma((7,)),
            dma((4, chips * 5)),
            dma((4, chips)),
            dma((4, chips)),
            dma((4,)),
            dma((chips,)),
            dma((chips,)),
            dma((chips,)),
            dma((chips,)),
            dma((ITERS - 1, 2)),
            dma((ITERS - 1, 2)),
            dma((n,)),
            dma((n,)),
            dma((5,)),
        ],
        compiler_params=pltpu.CompilerParams(
            collective_id=0, has_side_effects=True, vmem_limit_bytes=67_000_000
        ),
        name="segments",
    )(
        tokens,
        memory,
        norm_gain,
        post_gain,
        query_weight,
        key_matrix,
        value_matrix,
        output_weight,
        segment_weight,
    )
    return outs[0], outs[1], outs[2][0, :ITERS]


def solution(mesh):
    def step(*args):
        if fits(*args):
            return fused(*args)
        return shards(*args)

    in_specs = (
        P("seg", None),
        P(),
        P(),
        P(),
        P("seg", None),
        P(),
        P(),
        P("seg", None),
        P("seg"),
    )
    out_specs = (P("seg", None), P("seg", None), P())
    return jax.shard_map(
        step, mesh=mesh, in_specs=in_specs, out_specs=out_specs, check_vma=False
    )
```
